32 devices in a mesh: px: 4 (over x, core), py: 2 (over y), pz: 4 (over z).
Axes of the slice: x: 2, y: 2, z: 4, core: 2. Of those that a mesh axis runs over, the one named last changes fastest.
Arguments:
- control_values: float32 [28, 14, 28, 512], P('px', 'py', 'pz'), may hold values from -6 to 6
- metric_diag: float32 [3, 32, 512], P(None, 'px', ('py', 'pz')), may hold values from 0.5 to 2
- metric_off: float32 [3, 32, 512], P(None, 'px', ('py', 'pz')), may hold values from -0.2 to 0.2
- mass_weight: float32 [32, 512], P('px', ('py', 'pz')), may hold values from 0.5 to 2
- orient: int32 [4, 2, 4, 3], P('px', 'py', 'pz'), may hold values from 0 to 1
Outputs:
- stiffness_out: float32 [28, 14, 28, 512], P('px', 'py', 'pz')
- mass_out: float32 [28, 14, 28, 512], P('px', 'py', 'pz')
The draws below stay inside these ranges and needn't reach their ends.
All inputs are finite; a program needn't handle non-finite values.
Results may differ from the reference program's by a relative error of at most 0.0003.
Values sent between devices are 32-bit elements; how exact they have to be, the bound alone decides.
A program may use at most 64 MiB of HBM per device.

```python
import math
import jax
import jax.numpy as jnp
import numpy as np
from jax import lax

ELEMS = 4
VECS = 512
CTRL = 7
QUAD = 8
N_PX = 4
N_PY = 2
N_PZ = 4


def touch_ends(drawn, own_key, smallest, top_value):
    shape = drawn.shape
    index_at = [jax.random.randint(jax.random.fold_in(own_key, axis), (), 0, shape[axis]) for axis in range(len(shape))]
    drawn = drawn.at[tuple(index_at)].set(smallest)
    longest = shape.index(max(shape))
    index_at[longest] = (index_at[longest] + 1) % shape[longest]
    return drawn.at[tuple(index_at)].set(top_value)


def levels(rng, dims, split, least, high):
    loudness = 1.0
    for axis_at, blocks in split:
        draws = jax.random.uniform(jax.random.fold_in(jax.random.fold_in(rng, 6), axis_at), (blocks,), jnp.float32, least / len(split), high / len(split))
        loudness = loudness * jnp.repeat(jnp.exp(draws), dims[axis_at] // blocks).reshape((-1,) + (1,) * (len(dims) - 1 - axis_at))
    return loudness


def bell_draw(stream_key, shape, deviation, most, split=(), held_as=jnp.bfloat16):
    result = deviation * jax.random.normal(stream_key, shape, jnp.float32)
    if split:
        result = result * levels(stream_key, shape, split, -0.22, 0.18)
    return jnp.clip(result, -most, most).astype(held_as)


def setup_inputs(seed: int = 0) -> dict:
    key_of = jax.random.split(jax.random.key(seed), 6)
    return {
        "control_values": bell_draw(key_of[0], (N_PX * CTRL, N_PY * CTRL, N_PZ * CTRL, VECS), 1.0, 6.0, ((0, 4), (1, 2), (2, 4)), jnp.float32),
        "metric_diag": jnp.clip(jnp.exp(math.log(2.0) - 1.3862944 * jax.random.uniform(key_of[1], (3, N_PX * QUAD, N_PY * N_PZ * QUAD * QUAD), jnp.float32) ** levels(key_of[1], (3, N_PX * QUAD, N_PY * N_PZ * QUAD * QUAD), ((1, 4), (2, 8)), -0.2, 0.2)), 0.5, 2.0),
        "metric_off": jnp.clip(jax.random.uniform(key_of[2], (3, N_PX * QUAD, N_PY * N_PZ * QUAD * QUAD), jnp.float32, -0.2, 0.2) * levels(key_of[2], (3, N_PX * QUAD, N_PY * N_PZ * QUAD * QUAD), ((1, 4), (2, 8)), -0.4, 0.0), -0.2, 0.2),
        "mass_weight": jnp.clip(jnp.exp(math.log(2.0) - 1.3862944 * jax.random.uniform(key_of[3], (N_PX * QUAD, N_PY * N_PZ * QUAD * QUAD), jnp.float32) ** levels(key_of[3], (N_PX * QUAD, N_PY * N_PZ * QUAD * QUAD), ((0, 4), (1, 8)), -0.2, 0.2)), 0.5, 2.0),
        "orient": touch_ends(jax.random.randint(key_of[4], (N_PX, N_PY, N_PZ, 3), 0, 2), jax.random.fold_in(key_of[4], 1), 0, 1).astype(jnp.int32),
    }


def spline_tables(elements):
    knot_row = np.concatenate([np.zeros(3), np.arange(elements + 1) * 1.0, np.full(3, float(elements))])
    offsets = np.array([0.5 - 0.5 / math.sqrt(3.0), 0.5 + 0.5 / math.sqrt(3.0)])
    points = (np.arange(elements)[:, None] + offsets[None, :]).reshape(-1)
    intervals = np.repeat(np.arange(elements), 2) + 3
    current = np.zeros((points.size, knot_row.size - 1))
    current[np.arange(points.size), intervals] = 1.0
    previous = current
    for degree in range(1, 4):
        columns = knot_row.size - 1 - degree
        updated = np.zeros((points.size, columns))
        for i in range(columns):
            lower_gap = knot_row[i + degree] - knot_row[i]
            upper_gap = knot_row[i + degree + 1] - knot_row[i + 1]
            if lower_gap > 0:
                updated[:, i] += (points - knot_row[i]) / lower_gap * current[:, i]
            if upper_gap > 0:
                updated[:, i] += (knot_row[i + degree + 1] - points) / upper_gap * current[:, i + 1]
        previous = current
        current = updated
    slopes = np.zeros(current.shape)
    for i in range(current.shape[1]):
        lower_gap = knot_row[i + 3] - knot_row[i]
        upper_gap = knot_row[i + 4] - knot_row[i + 1]
        if lower_gap > 0:
            slopes[:, i] += 3.0 / lower_gap * previous[:, i]
        if upper_gap > 0:
            slopes[:, i] -= 3.0 / upper_gap * previous[:, i + 1]
    return (current.astype(np.float32), slopes.astype(np.float32))

def contract(pattern, operand, table_part):
    return jnp.einsum(pattern, operand, table_part, precision=lax.Precision.HIGHEST)

def forward_parts(coeffs, values, slopes):
    along_b = contract('ijkv,ck->ijcv', coeffs, values)
    along_d = contract('ijkv,ck->ijcv', coeffs, slopes)
    plain = contract('ijcv,bj->ibcv', along_b, values)
    slope_y = contract('ijcv,bj->ibcv', along_b, slopes)
    slope_z = contract('ijcv,bj->ibcv', along_d, values)
    return (plain, slope_y, slope_z)

def stiffness_apply(parts, diag_terms, off_terms, values, slopes, block_rows):
    plain, slope_y, slope_z = parts
    quad_count = values.shape[0]
    back_x = jnp.zeros(plain.shape, jnp.float32)
    back_y = jnp.zeros(plain.shape, jnp.float32)
    back_z = jnp.zeros(plain.shape, jnp.float32)
    for first_row in range(0, quad_count, block_rows):
        last_row = first_row + block_rows
        slope_rows = slopes[first_row:last_row]
        value_rows = values[first_row:last_row]
        grad_x = contract('ibcv,ai->abcv', plain, slope_rows)
        grad_y = contract('ibcv,ai->abcv', slope_y, value_rows)
        grad_z = contract('ibcv,ai->abcv', slope_z, value_rows)
        diag_rows = diag_terms[:, first_row:last_row, :, :, None]
        off_rows = off_terms[:, first_row:last_row, :, :, None]
        flux_x = diag_rows[0] * grad_x + off_rows[0] * grad_y + off_rows[1] * grad_z
        flux_y = off_rows[0] * grad_x + diag_rows[1] * grad_y + off_rows[2] * grad_z
        flux_z = off_rows[1] * grad_x + off_rows[2] * grad_y + diag_rows[2] * grad_z
        back_x = back_x + contract('abcv,ai->ibcv', flux_x, slope_rows)
        back_y = back_y + contract('abcv,ai->ibcv', flux_y, value_rows)
        back_z = back_z + contract('abcv,ai->ibcv', flux_z, value_rows)
    middle_b = contract('ibcv,bj->ijcv', back_x, values) + contract('ibcv,bj->ijcv', back_y, slopes)
    middle_d = contract('ibcv,bj->ijcv', back_z, values)
    return contract('ijcv,ck->ijkv', middle_b, values) + contract('ijcv,ck->ijkv', middle_d, slopes)

def mass_apply(plain, weights, values, block_rows):
    quad_count = values.shape[0]
    back_mass = jnp.zeros(plain.shape, jnp.float32)
    for first_row in range(0, quad_count, block_rows):
        last_row = first_row + block_rows
        value_rows = values[first_row:last_row]
        point_values = contract('ibcv,ai->abcv', plain, value_rows)
        weighted = weights[first_row:last_row, :, :, None] * point_values
        back_mass = back_mass + contract('abcv,ai->ibcv', weighted, value_rows)
    middle = contract('ibcv,bj->ijcv', back_mass, values)
    return contract('ijcv,ck->ijkv', middle, values)

def flip_frame(grid_data, flip_flags, first_dim):
    for d in range(3):
        grid_data = jnp.where(flip_flags[d] == 1, jnp.flip(grid_data, axis=first_dim + d), grid_data)
    return grid_data

def fold_axis(grid_data, patch_axis, point_axis):
    extent = grid_data.shape[point_axis]
    first_plane = lax.slice_in_dim(grid_data, 0, 1, axis=point_axis)
    last_plane = lax.slice_in_dim(grid_data, extent - 1, extent, axis=point_axis)
    middle = lax.slice_in_dim(grid_data, 1, extent - 1, axis=point_axis)
    from_before = jnp.roll(last_plane, 1, axis=patch_axis)
    from_after = jnp.roll(first_plane, -1, axis=patch_axis)
    return jnp.concatenate([first_plane + from_before, middle, last_plane + from_after], axis=point_axis)

def reference(control_values, metric_diag, metric_off, mass_weight, orient):
    values_np, slopes_np = spline_tables(ELEMS)
    values = jnp.asarray(values_np)
    slopes = jnp.asarray(slopes_np)
    patches = N_PX * N_PY * N_PZ
    coeffs = control_values.reshape(N_PX, CTRL, N_PY, CTRL, N_PZ, CTRL, VECS)
    coeffs = coeffs.transpose(0, 2, 4, 1, 3, 5, 6).reshape(patches, CTRL, CTRL, CTRL, VECS)
    diag_all = metric_diag.reshape(3, N_PX, QUAD, N_PY, N_PZ, QUAD, QUAD)
    diag_all = diag_all.transpose(1, 3, 4, 0, 2, 5, 6).reshape(patches, 3, QUAD, QUAD, QUAD)
    off_all = metric_off.reshape(3, N_PX, QUAD, N_PY, N_PZ, QUAD, QUAD)
    off_all = off_all.transpose(1, 3, 4, 0, 2, 5, 6).reshape(patches, 3, QUAD, QUAD, QUAD)
    weight_all = mass_weight.reshape(N_PX, QUAD, N_PY, N_PZ, QUAD, QUAD)
    weight_all = weight_all.transpose(0, 2, 3, 1, 4, 5).reshape(patches, QUAD, QUAD, QUAD)
    flag_all = orient.reshape(patches, 3)

    def one_patch(patch_items):
        coeff_patch, diag_patch, off_patch, weight_patch, flag_patch = patch_items
        parts = forward_parts(coeff_patch, values, slopes)
        stiffness = stiffness_apply(parts, diag_patch, off_patch, values, slopes, QUAD)
        mass_part = mass_apply(parts[0], weight_patch, values, QUAD)
        return (flip_frame(stiffness, flag_patch, 0), flip_frame(mass_part, flag_patch, 0))
    stiffness_all, mass_all = lax.map(one_patch, (coeffs, diag_all, off_all, weight_all, flag_all))

    def assemble(grid_data):
        grid_data = grid_data.reshape(N_PX, N_PY, N_PZ, CTRL, CTRL, CTRL, VECS)
        grid_data = fold_axis(grid_data, 0, 3)
        grid_data = fold_axis(grid_data, 1, 4)
        grid_data = fold_axis(grid_data, 2, 5)
        return grid_data.reshape(patches, CTRL, CTRL, CTRL, VECS)

    def flip_back(patch_items):
        stiff_patch, mass_patch, flag_patch = patch_items
        return (flip_frame(stiff_patch, flag_patch, 0), flip_frame(mass_patch, flag_patch, 0))
    stiffness_all, mass_all = lax.map(flip_back, (assemble(stiffness_all), assemble(mass_all), flag_all))

    def to_layout(grid_data):
        grid_data = grid_data.reshape(N_PX, N_PY, N_PZ, CTRL, CTRL, CTRL, VECS)
        return grid_data.transpose(0, 3, 1, 4, 2, 5, 6).reshape(N_PX * CTRL, N_PY * CTRL, N_PZ * CTRL, VECS)
    return (to_layout(stiffness_all), to_layout(mass_all))
```

```python
import functools
import heapq
import math

import jax
import jax.numpy as jnp
import numpy as np
from jax import lax
from jax.experimental import pallas as pl
from jax.experimental.pallas import tpu as pltpu
from jax.sharding import PartitionSpec as P

LANES = 128
ROWS = 8
AXES = ("px", "py", "pz")


def spline_tables(elements):
    knot_row = np.concatenate(
        [np.zeros(3), np.arange(elements + 1) * 1.0, np.full(3, float(elements))]
    )
    offsets = np.array([0.5 - 0.5 / math.sqrt(3.0), 0.5 + 0.5 / math.sqrt(3.0)])
    points = (np.arange(elements)[:, None] + offsets[None, :]).reshape(-1)
    intervals = np.repeat(np.arange(elements), 2) + 3
    current = np.zeros((points.size, knot_row.size - 1))
    current[np.arange(points.size), intervals] = 1.0
    previous = current
    for degree in range(1, 4):
        columns = knot_row.size - 1 - degree
        updated = np.zeros((points.size, columns))
        for i in range(columns):
            lower_gap = knot_row[i + degree] - knot_row[i]
            upper_gap = knot_row[i + degree + 1] - knot_row[i + 1]
            if lower_gap > 0:
                updated[:, i] += (points - knot_row[i]) / lower_gap * current[:, i]
            if upper_gap > 0:
                updated[:, i] += (knot_row[i + degree + 1] - points) / upper_gap * current[:, i + 1]
        previous = current
        current = updated
    slopes = np.zeros(current.shape)
    for i in range(current.shape[1]):
        lower_gap = knot_row[i + 3] - knot_row[i]
        upper_gap = knot_row[i + 4] - knot_row[i + 1]
        if lower_gap > 0:
            slopes[:, i] += 3.0 / lower_gap * previous[:, i]
        if upper_gap > 0:
            slopes[:, i] -= 3.0 / upper_gap * previous[:, i + 1]
    return (current.astype(np.float32), slopes.astype(np.float32))


def split(x):
    high = x.astype(jnp.bfloat16)
    return high, (x - high.astype(jnp.float32)).astype(jnp.bfloat16)


def split_table(table):
    high = table.astype(jnp.bfloat16)
    low = (table - high.astype(np.float32)).astype(jnp.bfloat16)
    return np.asarray(high), np.asarray(low)


def plane_tables(values, slopes):
    quad, ctrl = values.shape
    wide = np.zeros((quad, ROWS), np.float64)
    tall = np.zeros((quad, ROWS), np.float64)
    wide[:, :ctrl] = values
    tall[:, :ctrl] = slopes
    fields = [np.kron(wide, wide), np.kron(tall, wide), np.kron(wide, tall)]
    forward = np.concatenate(fields, 0).astype(np.float32)
    high, low = split_table(forward)
    forward = np.concatenate([high, high, low], 1)
    backward = []
    size = ctrl * ROWS
    for flip_y in range(2):
        for flip_z in range(2):
            rows = np.full(size, -1)
            for j in range(ctrl):
                for k in range(ctrl):
                    jj = ctrl - 1 - j if flip_y else j
                    kk = ctrl - 1 - k if flip_z else k
                    rows[j * ROWS + k] = jj * ROWS + kk
            back = [np.where(rows[:, None] >= 0, f.T[rows], 0.0) for f in fields]
            none = np.zeros_like(back[0])
            stiff = np.concatenate([back[0], back[1], back[2], none], 1)
            mass = np.concatenate([none, none, none, back[0]], 1)
            backward.append(np.concatenate([stiff, mass], 0).astype(np.float32))
    return forward, np.stack(backward)


def make_copies(orders, zsend, bufs, state, send_sem, recv_sem, nbrs, c, stage):
    ctrl = state.shape[2]
    d = orders[c % len(orders)][stage]
    result = []
    for side in range(2):
        e = side * (ctrl - 1)
        if d == 0:
            plane = state.at[c, :, e]
        elif d == 1:
            plane = state.at[c, :, :, e * ROWS : e * ROWS + ctrl]
        else:
            plane = zsend.at[c, side]
        result.append(
            pltpu.make_async_remote_copy(
                src_ref=plane,
                dst_ref=bufs[d].at[c, 1 - side],
                send_sem=send_sem.at[c, d, side],
                recv_sem=recv_sem.at[c, d, 1 - side],
                device_id={AXES[d]: nbrs[d][side]},
                device_id_type=pl.DeviceIdType.MESH,
            )
        )
    return result


def patch_kernel(
    values, slopes, orient, u_hbm, diag_ref, off_ref, weight_ref, fwd_ref, bwd_ref,
    stiff_out, mass_out,
    ubuf, upad, square, coef, fields, back, table, state, xbuf, ybuf, zbuf, zsend,
    u_sem, send_sem, recv_sem,
):
    quad, ctrl = values.shape
    vecs = u_hbm.shape[3]
    halves, width = ubuf.shape[0], ubuf.shape[4]
    chunks = vecs // LANES
    per_half = width // LANES
    points = quad * quad
    size = ctrl * ROWS
    bufs = (xbuf, ybuf, zbuf)

    loads = [
        pltpu.make_async_copy(
            u_hbm.at[:, :, :, h * width : (h + 1) * width], ubuf.at[h], u_sem.at[h]
        )
        for h in range(halves)
    ]
    for load in loads:
        load.start()

    nbrs = []
    for axis in AXES:
        count, me = lax.axis_size(axis), lax.axis_index(axis)
        nbrs.append((lax.rem(me + count - 1, count), lax.rem(me + 1, count)))
    barrier = pltpu.get_barrier_semaphore()
    for d in range(3):
        for side in range(2):
            pl.semaphore_signal(
                barrier,
                inc=1,
                device_id={AXES[d]: nbrs[d][side]},
                device_id_type=pl.DeviceIdType.MESH,
            )

    upad[...] = jnp.zeros_like(upad)
    square[...] = jnp.zeros_like(square)
    for s in range(3):
        square[s * quad : (s + 1) * quad, 0:points] = diag_ref[s]
        square[(3 + s) * quad : (4 + s) * quad, 0:points] = off_ref[s]
    square[6 * quad : 7 * quad, 0:points] = weight_ref[...]
    across = square[...].T
    for c in range(7 * quad):
        coef[c] = jnp.broadcast_to(across[0:points, c : c + 1], (points, LANES))

    def flips(shape):
        return [jnp.full(shape, orient[d], jnp.int32) == 1 for d in range(3)]

    _, flip_y, flip_z = flips(bwd_ref.shape[1:])
    high, low = split(
        jnp.where(
            flip_y,
            jnp.where(flip_z, bwd_ref[3], bwd_ref[2]),
            jnp.where(flip_z, bwd_ref[1], bwd_ref[0]),
        )
    )
    table[0 : 2 * size] = high
    table[2 * size : 4 * size] = low

    def operate(h):
        for i in range(ctrl):
            upad[i % 2, 0:ctrl, 0:ctrl, :] = ubuf[h, i]
            high, low = split(upad[i % 2].reshape(ROWS * ROWS, width))
            stacked = jnp.concatenate([high, low, high], axis=0)
            fields[i] = jnp.dot(fwd_ref[...], stacked, preferred_element_type=jnp.float32)

        @pl.loop(0, quad)
        def _(b):
            row = pl.multiple_of(b * ROWS, ROWS)
            for l in range(per_half):
                lanes = slice(l * LANES, (l + 1) * LANES)
                part = [
                    [fields[i, pl.ds(f * points + row, ROWS), lanes] for f in range(3)]
                    for i in range(ctrl)
                ]
                acc = [[None] * ctrl for _ in range(4)]
                for q in range(quad):
                    near = [i for i in range(ctrl) if values[q, i] != 0.0 or slopes[q, i] != 0.0]
                    v = {i: float(values[q, i]) for i in near}
                    s = {i: float(slopes[q, i]) for i in near}
                    g1 = sum(s[i] * part[i][0] for i in near)
                    p = sum(v[i] * part[i][0] for i in near)
                    g2 = sum(v[i] * part[i][1] for i in near)
                    g3 = sum(v[i] * part[i][2] for i in near)
                    d = [coef[t * quad + q, pl.ds(row, ROWS), :] for t in range(7)]
                    flux = [
                        d[0] * g1 + d[3] * g2 + d[4] * g3,
                        d[3] * g1 + d[1] * g2 + d[5] * g3,
                        d[4] * g1 + d[5] * g2 + d[2] * g3,
                        d[6] * p,
                    ]
                    for f in range(4):
                        for i in near:
                            term = (s[i] if f == 0 else v[i]) * flux[f]
                            acc[f][i] = term if acc[f][i] is None else acc[f][i] + term
                for f in range(4):
                    for i in range(ctrl):
                        back[i, pl.ds(f * points + row, ROWS), lanes] = acc[f][i]

        flip = flips((4 * points, width))[0]
        for i in range(ctrl):
            high, low = split(jnp.where(flip, back[ctrl - 1 - i], back[i]))
            both = jnp.dot(table[...], high, preferred_element_type=jnp.float32)
            rest = jnp.dot(table[0 : 2 * size], low, preferred_element_type=jnp.float32)
            total = both[0 : 2 * size] + both[2 * size : 4 * size] + rest
            for f in range(2):
                for l in range(per_half):
                    lanes = slice(l * LANES, (l + 1) * LANES)
                    state[h * per_half + l, f, i] = total[f * size : (f + 1) * size, lanes]

    copies = functools.partial(
        make_copies, ORDERS, zsend, bufs, state, send_sem, recv_sem, nbrs
    )

    def start(c, stage):
        if ORDERS[c % len(ORDERS)][stage] == 2:
            for side in range(2):
                for f in range(2):
                    for i in range(ctrl):
                        rows = pl.ds(side * (ctrl - 1), ctrl, stride=ROWS)
                        zsend[c, side, f, i] = state[c, f, i, rows, :]
        for copy in copies(c, stage):
            copy.start()

    index = lax.broadcasted_iota(jnp.int32, (ROWS, LANES), 0)
    index = jnp.maximum(ctrl - 1 - index, 0)
    flip_x, flip_y, flip_z = flips((ROWS, LANES))
    for c, stage in exchange_plan(chunks, per_half):
        if stage < 0:
            loads[c].wait()
            operate(c)
            if c == 0:
                pl.semaphore_wait(barrier, 6)
            for l in range(per_half):
                start(c * per_half + l, 0)
            continue
        d = ORDERS[c % len(ORDERS)][stage]
        for copy in copies(c, stage):
            copy.wait()
        for side in range(2):
            e = side * (ctrl - 1)
            for f in range(2):
                if d == 0:
                    state[c, f, e] += xbuf[c, side, f]
                    continue
                for i in range(ctrl):
                    if d == 1:
                        state[c, f, i, e * ROWS : e * ROWS + ctrl] += ybuf[c, side, f, i]
                    else:
                        rows = pl.ds(e, ctrl, stride=ROWS)
                        state[c, f, i, rows, :] = state[c, f, i, rows, :] + zbuf[c, side, f, i]
        if stage < 2:
            start(c, stage + 1)
            continue
        lanes = slice(c * LANES, (c + 1) * LANES)
        for f in range(2):
            for i in range(ctrl):
                for j in range(ctrl):
                    x = [
                        [state[c, f, ii, jj * ROWS : (jj + 1) * ROWS] for jj in (j, ctrl - 1 - j)]
                        for ii in (i, ctrl - 1 - i)
                    ]
                    x = [jnp.where(flip_y, y[1], y[0]) for y in x]
                    x = jnp.where(flip_x, x[1], x[0])
                    other = jnp.take_along_axis(x, index, axis=0, mode="promise_in_bounds")
                    (stiff_out, mass_out)[f][i, j, :, lanes] = jnp.where(flip_z, other, x)[0:ctrl]


ORDERS = ((0, 2, 1), (1, 0, 2), (0, 2, 1), (1, 0, 2))
WIRE = (1.23, 2.15, 2.15)
LATENCY = (2.2, 2.2, 3.4)
COMPUTE = 1.7
FOLD = 0.3


def exchange_plan(chunks, per_part):
    free = [0.0, 0.0, 0.0]
    heap, plan = [], []

    def send(time, chunk, stage):
        d = ORDERS[chunk % len(ORDERS)][stage]
        free[d] = max(free[d], time) + WIRE[d]
        heapq.heappush(heap, (free[d] + LATENCY[d], chunk, stage))

    def arrivals(now, limit):
        while heap and heap[0][0] <= limit:
            time, chunk, stage = heapq.heappop(heap)
            now = max(now, time) + FOLD
            plan.append((chunk, stage))
            if stage < 2:
                send(now, chunk, stage + 1)
        return now

    now = 0.0
    for part in range(chunks // per_part):
        now = arrivals(now, now) + COMPUTE * per_part
        plan.append((part, -1))
        for chunk in range(part * per_part, (part + 1) * per_part):
            send(now, chunk, 0)
    arrivals(now, math.inf)
    return plan


def apply_patch(u, diag, off, weight, orient, values, slopes):
    quad, ctrl = values.shape
    vecs = u.shape[3]
    width = 2 * LANES
    halves = vecs // width
    chunks = vecs // LANES
    points = quad * quad
    size = ctrl * ROWS
    forward, backward = plane_tables(values, slopes)
    vmem = pl.BlockSpec(memory_space=pltpu.VMEM)
    hbm = pl.BlockSpec(memory_space=pl.ANY)
    f32 = jnp.float32
    return pl.pallas_call(
        functools.partial(patch_kernel, values, slopes),
        out_shape=[pltpu.VMEM(u.shape, f32)] * 2,
        in_specs=[pl.BlockSpec(memory_space=pltpu.SMEM), hbm] + [vmem] * 5,
        out_specs=[vmem, vmem],
        scratch_shapes=[
            pltpu.VMEM((halves, ctrl, ctrl, ctrl, width), f32),
            pltpu.VMEM((2, ROWS, ROWS, width), f32),
            pltpu.VMEM((LANES, LANES), f32),
            pltpu.VMEM((7 * quad, points, LANES), f32),
            pltpu.VMEM((ctrl, 3 * points, width), f32),
            pltpu.VMEM((ctrl, 4 * points, width), f32),
            pltpu.VMEM((4 * size, 4 * points), jnp.bfloat16),
            pltpu.VMEM((chunks, 2, ctrl, size, LANES), f32),
            pltpu.VMEM((chunks, 2, 2, size, LANES), f32),
            pltpu.VMEM((chunks, 2, 2, ctrl, ctrl, LANES), f32),
            pltpu.VMEM((chunks, 2, 2, ctrl, ctrl, LANES), f32),
            pltpu.VMEM((chunks, 2, 2, ctrl, ctrl, LANES), f32),
            pltpu.SemaphoreType.DMA((halves,)),
            pltpu.SemaphoreType.DMA((chunks, 3, 2)),
            pltpu.SemaphoreType.DMA((chunks, 3, 2)),
        ],
        compiler_params=pltpu.CompilerParams(collective_id=0, has_side_effects=True),
        name="apply_patch",
    )(orient, u, diag, off, weight, jnp.asarray(forward), jnp.asarray(backward))


def store_kernel(stiff, mass, stiff_out, mass_out, sem):
    copies = [
        pltpu.make_async_copy((stiff, mass)[f].at[i], (stiff_out, mass_out)[f].at[i], sem.at[f, i])
        for f in range(2)
        for i in range(stiff.shape[0])
    ]
    for copy in copies:
        copy.start()
    for copy in copies:
        copy.wait()


def store_results(stiff, mass):
    vmem = pl.BlockSpec(memory_space=pltpu.VMEM)
    hbm = pl.BlockSpec(memory_space=pl.ANY)
    return pl.pallas_call(
        store_kernel,
        out_shape=[jax.ShapeDtypeStruct(stiff.shape, stiff.dtype)] * 2,
        in_specs=[vmem, vmem],
        out_specs=[hbm, hbm],
        scratch_shapes=[pltpu.SemaphoreType.DMA((2, stiff.shape[0]))],
        name="store_results",
    )(*(pltpu.with_memory_space_constraint(x, pltpu.VMEM) for x in (stiff, mass)))


def per_device(control_values, metric_diag, metric_off, mass_weight, orient):
    values, slopes = spline_tables(mass_weight.shape[0] // 2)
    stiff, mass = apply_patch(
        control_values, metric_diag, metric_off, mass_weight, orient.reshape(3), values, slopes
    )
    return tuple(store_results(stiff, mass))


def solution(mesh):
    in_specs = (
        P("px", "py", "pz", None),
        P(None, "px", ("py", "pz")),
        P(None, "px", ("py", "pz")),
        P("px", ("py", "pz")),
        P("px", "py", "pz", None),
    )
    out_specs = (P("px", "py", "pz", None), P("px", "py", "pz", None))
    return jax.shard_map(
        per_device, mesh=mesh, in_specs=in_specs, out_specs=out_specs, check_vma=False
    )
```

```python
import functools
import heapq
import itertools
import math
from typing import NamedTuple

import jax
import jax.numpy as jnp
import numpy as np
from jax import lax
from jax.experimental import pallas as pl
from jax.experimental.pallas import tpu as pltpu
from jax.sharding import PartitionSpec as P

LANES = 128
ROWS = 8
AXES = ("px", "py", "pz")


def spline_tables(elements):
    knot_row = np.concatenate(
        [np.zeros(3), np.arange(elements + 1) * 1.0, np.full(3, float(elements))]
    )
    offsets = np.array([0.5 - 0.5 / math.sqrt(3.0), 0.5 + 0.5 / math.sqrt(3.0)])
    points = (np.arange(elements)[:, None] + offsets[None, :]).reshape(-1)
    intervals = np.repeat(np.arange(elements), 2) + 3
    current = np.zeros((points.size, knot_row.size - 1))
    current[np.arange(points.size), intervals] = 1.0
    previous = current
    for degree in range(1, 4):
        columns = knot_row.size - 1 - degree
        updated = np.zeros((points.size, columns))
        for i in range(columns):
            lower_gap = knot_row[i + degree] - knot_row[i]
            upper_gap = knot_row[i + degree + 1] - knot_row[i + 1]
            if lower_gap > 0:
                updated[:, i] += (points - knot_row[i]) / lower_gap * current[:, i]
            if upper_gap > 0:
                updated[:, i] += (knot_row[i + degree + 1] - points) / upper_gap * current[:, i + 1]
        previous = current
        current = updated
    slopes = np.zeros(current.shape)
    for i in range(current.shape[1]):
        lower_gap = knot_row[i + 3] - knot_row[i]
        upper_gap = knot_row[i + 4] - knot_row[i + 1]
        if lower_gap > 0:
            slopes[:, i] += 3.0 / lower_gap * previous[:, i]
        if upper_gap > 0:
            slopes[:, i] -= 3.0 / upper_gap * previous[:, i + 1]
    return (current.astype(np.float32), slopes.astype(np.float32))


def split(x):
    high = x.astype(jnp.bfloat16)
    return high, (x - high.astype(jnp.float32)).astype(jnp.bfloat16)


def split_table(table):
    high = table.astype(jnp.bfloat16)
    low = (table - high.astype(np.float32)).astype(jnp.bfloat16)
    return np.asarray(high), np.asarray(low)


def place(index, ctrl):
    return (0, *range(2, ctrl), 1)[index]


def plane_tables(values, slopes):
    quad, ctrl = values.shape
    wide = np.zeros((quad, ROWS), np.float64)
    tall = np.zeros((quad, ROWS), np.float64)
    wide[:, :ctrl] = values
    tall[:, :ctrl] = slopes
    fields = [np.kron(wide, wide), np.kron(tall, wide), np.kron(wide, tall)]
    forward = np.concatenate(fields, 0).astype(np.float32)
    high, low = split_table(forward)
    forward = np.concatenate([high, high, low], 1)
    backward = []
    size = ctrl * ROWS
    for flip_y in range(2):
        for flip_z in range(2):
            rows = np.full(size, -1)
            for j in range(ctrl):
                for k in range(ctrl):
                    jj = ctrl - 1 - j if flip_y else j
                    kk = ctrl - 1 - k if flip_z else k
                    rows[place(j, ctrl) * ROWS + k] = jj * ROWS + kk
            back = [np.where(rows[:, None] >= 0, f.T[rows], 0.0) for f in fields]
            none = np.zeros_like(back[0])
            stiff = np.concatenate([back[0], back[1], back[2], none], 1)
            mass = np.concatenate([none, none, none, back[0]], 1)
            backward.append(np.concatenate([stiff, mass], 0).astype(np.float32))
    return forward, np.stack(backward)


def point_scales(values, slopes):
    v = np.take_along_axis(values, np.abs(values).argmax(1)[:, None], 1)[:, 0]
    s = np.take_along_axis(slopes, np.abs(slopes).argmax(1)[:, None], 1)[:, 0]
    v, s = v.astype(np.float64), s.astype(np.float64)
    scales = np.stack([s * s, v * v, v * v, s * v, s * v, v * v, v * v])
    return v, s, scales.astype(np.float32)


def combine(weights, terms):
    total = None
    for weight, term in zip(weights, terms):
        term = term if weight == 1.0 else weight * term
        total = term if total is None else total + term
    return total


ENDS, INNER, ALL = slice(0, 2), slice(2, None), slice(None)


def span(planes, ctrl):
    return range(ctrl)[planes]


class Move(NamedTuple):
    axes: tuple
    x: slice | None
    y: slice | None
    after: tuple = ()

    def points(self, ctrl):
        sizes = [len(span(planes, ctrl)) for planes in (self.x, self.y) if planes is not None]
        return math.prod(sizes) * {(0,): ROWS, (1,): ctrl}.get(self.axes, 1)


CHAIN = (
    Move((0,), None, ALL),
    Move((1,), INNER, None),
    Move((2,), INNER, INNER),
    Move((1,), ENDS, None, (0,)),
    Move((2,), ENDS, INNER, (0,)),
    Move((2,), ALL, ENDS, (1, 3)),
)
DIRECT = (
    Move((0,), None, ALL),
    Move((1, 2), INNER, None),
    Move((1,), INNER, None),
    Move((2,), INNER, ALL),
    Move((1, 2), ENDS, None, (0,)),
    Move((1,), ENDS, None, (0,)),
    Move((2,), ENDS, ALL, (0,)),
)
MOVES = (CHAIN, CHAIN, DIRECT, DIRECT)
SLOTS = max(len(moves) for moves in MOVES)


def sent_rows(ctrl):
    return sum(move.points(ctrl) * 2 ** len(move.axes) * 2 for moves in MOVES for move in moves)


class Exchange:
    def __init__(self, state, sends, bufs, tally, send_sem, recv_sem, nbrs):
        self.state, self.sends, self.bufs, self.tally = state, sends, bufs, tally
        self.send_sem, self.recv_sem, self.nbrs = send_sem, recv_sem, nbrs
        self.ctrl = state.shape[2]

    def parts(self, c, m):
        move, ctrl = MOVES[c][m], self.ctrl
        for f in range(2):
            for sides in itertools.product(range(2), repeat=len(move.axes)):
                if move.axes == (0,):
                    yield sides, (c, f, sides[0]), (c, *sides, f)
                    continue
                for n, i in enumerate(span(move.x, ctrl)):
                    if move.axes == (1,):
                        rows = pl.ds(sides[0] * ROWS, ctrl)
                        yield sides, (c, f, i, rows), (c, *sides, f, i)
                    elif move.axes == (2,):
                        y = span(move.y, ctrl)
                        start = y[0] * ROWS + sides[0] * (ctrl - 1)
                        rows = pl.ds(start, len(y), stride=ROWS)
                        yield sides, (c, f, i, rows), (c, *sides, f, i)
                    else:
                        row = sides[0] * ROWS + sides[1] * (ctrl - 1)
                        yield sides, (c, f, i, pl.ds(row, 1)), (c, *sides, f, pl.ds(n, 1))

    def view(self, bufs, c, m, sides):
        move = MOVES[c][m]
        index = (c, *sides) if sides else (c,) + (ALL,) * len(move.axes)
        if move.axes == (0,):
            return bufs[0].at[index]
        x = span(move.x, self.ctrl)
        if len(move.axes) == 1:
            index += (ALL, slice(x[0], x[-1] + 1))
        return self.buffer(bufs, move).at[index]

    def buffer(self, bufs, move):
        if move.axes == (2,):
            return bufs[2 + (INNER, ENDS, ALL).index(move.y)]
        if move.axes == (1, 2):
            return bufs[5 + (INNER, ENDS).index(move.x)]
        return bufs[move.axes[0]]

    def start(self, c, m):
        move = MOVES[c][m]
        send = self.buffer(self.sends, move)
        for _, here, there in self.parts(c, m):
            send[there] = self.state[here]
        for sides in itertools.product(range(2), repeat=len(move.axes)):
            opposite = tuple(1 - side for side in sides)
            pltpu.make_async_remote_copy(
                src_ref=self.view(self.sends, c, m, sides),
                dst_ref=self.view(self.bufs, c, m, opposite),
                send_sem=self.send_sem,
                recv_sem=self.recv_sem.at[c, m],
                device_id={AXES[a]: self.nbrs[a][side] for a, side in zip(move.axes, sides)},
                device_id_type=pl.DeviceIdType.MESH,
            ).start()

    def finish(self, c, m):
        move = MOVES[c][m]
        landed = self.view(self.bufs, c, m, None)
        pltpu.make_async_copy(landed, landed, self.recv_sem.at[c, m]).wait()
        buf = self.buffer(self.bufs, move)
        for _, here, there in self.parts(c, m):
            self.state[here] = self.state[here] + buf[there]

    def drain(self):
        pltpu.make_async_copy(self.tally, self.tally, self.send_sem).wait()


def patch_kernel(
    values, slopes, orient_hbm, u_hbm, diag_hbm, off_hbm, weight_hbm, scale_hbm, fwd_hbm, bwd_hbm,
    stiff_out, mass_out,
    orient, ubuf, metric, scale, fwd, bwd, square, coef, fields, back, table, state, sends, bufs,
    tally, u_sem, load_sem, send_sem, recv_sem,
):
    quad, ctrl = values.shape
    chunks = ubuf.shape[0]
    points = quad * quad
    size = ctrl * ROWS

    nbrs = []
    for axis in AXES:
        count, me = lax.axis_size(axis), lax.axis_index(axis)
        nbrs.append((lax.rem(me + count - 1, count), lax.rem(me + 1, count)))
    barrier = pltpu.get_barrier_semaphore()
    peers = [
        {AXES[a]: nbrs[a][side] for a, side in zip(axes, sides)}
        for axes in sorted({move.axes for moves in MOVES for move in moves})
        for sides in itertools.product(range(2), repeat=len(axes))
    ]
    for peer in peers:
        pl.semaphore_signal(barrier, inc=1, device_id=peer, device_id_type=pl.DeviceIdType.MESH)

    measures = [
        pltpu.make_async_copy(diag_hbm, metric.at[0:3], load_sem.at[0]),
        pltpu.make_async_copy(off_hbm, metric.at[3:6], load_sem.at[0]),
        pltpu.make_async_copy(weight_hbm, metric.at[6], load_sem.at[0]),
    ]
    loads = [
        pltpu.make_async_copy(
            u_hbm.at[:, :, :, c * LANES : (c + 1) * LANES], ubuf.at[c, :, :, 0:ctrl], u_sem.at[c]
        )
        for c in range(chunks)
    ]
    scale_load = pltpu.make_async_copy(scale_hbm, scale, load_sem.at[1])
    forward_load = pltpu.make_async_copy(fwd_hbm, fwd, load_sem.at[2])
    backward_loads = [
        pltpu.make_async_copy(bwd_hbm, bwd, load_sem.at[3]),
        pltpu.make_async_copy(orient_hbm, orient, load_sem.at[4]),
    ]
    for load in measures + [scale_load, loads[0], forward_load] + backward_loads + loads[1:]:
        load.start()

    square[...] = jnp.zeros_like(square)
    pltpu.make_async_copy(metric, metric, load_sem.at[0]).wait()
    scale_load.wait()
    for t in range(7):
        square[t * quad : (t + 1) * quad, 0:points] = metric[t] * scale[t]
    across = square[...].T
    for t in range(7 * quad):
        coef[t] = jnp.broadcast_to(across[0:points, t : t + 1], (points, LANES))
    forward_load.wait()
    for load in backward_loads:
        load.wait()

    def flips(shape):
        return [jnp.full(shape, orient[d], jnp.int32) == 1 for d in range(3)]

    _, flip_y, flip_z = flips((2 * size, 4 * points))
    high, low = split(
        jnp.where(flip_y, jnp.where(flip_z, bwd[3], bwd[2]), jnp.where(flip_z, bwd[1], bwd[0]))
    )
    columns = 4 * points
    table[:, 0:columns] = high
    table[:, columns : 2 * columns] = low
    table[:, 2 * columns : 3 * columns] = high
    flip_x, flip_y, flip_z = flips((ROWS, LANES))
    flip_block = flips((2 * size, LANES))[0]
    value_scale, slope_scale, _ = point_scales(values, slopes)

    def operate(c):
        for i in range(ctrl):
            ubuf[c, i, :, ctrl:ROWS, :] = jnp.zeros((ctrl, ROWS - ctrl, LANES), jnp.float32)
        none = jnp.zeros((ROWS * ROWS - size, LANES), jnp.float32)
        for i in range(0, ctrl, 2):
            pair = [p for p in (i, i + 1) if p < ctrl]
            planes = [
                jnp.concatenate([ubuf[c, p].reshape(size, LANES), none], axis=0) for p in pair
            ]
            high, low = split(jnp.concatenate(planes, axis=1))
            stacked = jnp.concatenate([high, low, high], axis=0)
            result = jnp.dot(fwd[...], stacked, preferred_element_type=jnp.float32)
            for n, p in enumerate(pair):
                fields[p] = result[:, n * LANES : (n + 1) * LANES]

        @pl.loop(0, quad)
        def _(b):
            row = pl.multiple_of(b * ROWS, ROWS)
            part = [
                [fields[i, pl.ds(f * points + row, ROWS), :] for f in range(3)]
                for i in range(ctrl)
            ]
            acc = [[None] * ctrl for _ in range(4)]
            for q in range(quad):
                near = [i for i in range(ctrl) if values[q, i] != 0.0 or slopes[q, i] != 0.0]
                v = [float(values[q, i] / value_scale[q]) for i in near]
                s = [float(slopes[q, i] / slope_scale[q]) for i in near]
                g1 = combine(s, [part[i][0] for i in near])
                p = combine(v, [part[i][0] for i in near])
                g2 = combine(v, [part[i][1] for i in near])
                g3 = combine(v, [part[i][2] for i in near])
                d = [coef[t * quad + q, pl.ds(row, ROWS), :] for t in range(7)]
                flux = [
                    d[0] * g1 + d[3] * g2 + d[4] * g3,
                    d[3] * g1 + d[1] * g2 + d[5] * g3,
                    d[4] * g1 + d[5] * g2 + d[2] * g3,
                    d[6] * p,
                ]
                for f in range(4):
                    for n, i in enumerate(near):
                        weight = s[n] if f == 0 else v[n]
                        term = flux[f] if weight == 1.0 else weight * flux[f]
                        acc[f][i] = term if acc[f][i] is None else acc[f][i] + term
            for f in range(4):
                for i in range(ctrl):
                    back[i, pl.ds(f * points + row, ROWS), :] = acc[f][i]

        for i in range((ctrl + 1) // 2):
            pair = [i, ctrl - 1 - i][: 1 if 2 * i == ctrl - 1 else 2]
            high, low = split(jnp.concatenate([back[p] for p in pair], axis=1))
            stacked = jnp.concatenate([high, high, low], axis=0)
            total = jnp.dot(table[...], stacked, preferred_element_type=jnp.float32)
            sums = [total[:, n * LANES : (n + 1) * LANES] for n in range(len(pair))]
            for p, own, other in zip(pair, sums, sums[::-1]):
                plane = own if len(pair) == 1 else jnp.where(flip_block, other, own)
                for f in range(2):
                    state[c, f, place(p, ctrl)] = plane[f * size : (f + 1) * size]

    exchange = Exchange(state, sends, bufs, tally, send_sem, recv_sem, nbrs)
    index = lax.broadcasted_iota(jnp.int32, (ROWS, LANES), 0)
    index = jnp.maximum(ctrl - 1 - index, 0)
    for step, c, m in exchange_plan(chunks, ctrl):
        if step == "compute":
            loads[c].wait()
            operate(c)
            if c == 0:
                pl.semaphore_wait(barrier, len(peers))
        if step == "start":
            exchange.start(c, m)
        if step == "finish":
            exchange.finish(c, m)
        if step != "final":
            continue
        lanes = slice(c * LANES, (c + 1) * LANES)
        for f, i, j in itertools.product(range(2), range(ctrl), range(ctrl)):
            x = [
                [
                    state[c, f, place(ii, ctrl), jj * ROWS : (jj + 1) * ROWS]
                    for jj in (place(j, ctrl), place(ctrl - 1 - j, ctrl))
                ]
                for ii in (i, ctrl - 1 - i)
            ]
            x = [jnp.where(flip_y, y[1], y[0]) for y in x]
            x = jnp.where(flip_x, x[1], x[0])
            other = jnp.take_along_axis(x, index, axis=0, mode="promise_in_bounds")
            (stiff_out, mass_out)[f][i, j, :, lanes] = jnp.where(flip_z, other, x)[0:ctrl]
    exchange.drain()


RATE = (0.022, 0.04, 0.04)
LATENCY = (1.8, 2.0, 2.5)
COMPUTE_TIME = 1.3
FOLD = 0.05
GRACE = 0.45
BEHIND = 1.0


def exchange_plan(chunks, ctrl):
    free = [0.0, 0.0, 0.0]
    pending, plan = [], []
    folded = [set() for _ in range(chunks)]
    started = [set() for _ in range(chunks)]

    def begin(time, chunk, axes=None):
        for m, move in enumerate(MOVES[chunk]):
            ready = folded[chunk].issuperset(move.after) and axes in (None, move.axes)
            if m in started[chunk] or not ready:
                continue
            started[chunk].add(m)
            plan.append(("start", chunk, m))
            cost = move.points(ctrl) * 2 ** (len(move.axes) - 1)
            for a in move.axes:
                free[a] = max(free[a], time) + cost * RATE[a]
            late = max(free[a] + LATENCY[a] for a in move.axes)
            late += BEHIND if 2 in move.axes else 0.0
            heapq.heappush(pending, (late, chunk, m))

    def arrivals(now, limit, along):
        kept = []
        while pending and pending[0][0] <= limit:
            time, chunk, m = heapq.heappop(pending)
            if MOVES[chunk][m].axes not in along:
                kept.append((time, chunk, m))
                continue
            now = max(now, time) + FOLD
            folded[chunk].add(m)
            plan.append(("finish", chunk, m))
            begin(now, chunk)
            if len(folded[chunk]) == len(MOVES[chunk]):
                plan.append(("final", chunk, None))
        for item in kept:
            heapq.heappush(pending, item)
        return now

    now = 0.0
    for chunk in range(chunks):
        now += COMPUTE_TIME
        plan.append(("compute", chunk, None))
        begin(now, chunk, (0,))
        if chunk == chunks - 1:
            now = arrivals(now, now + GRACE, ((0,), (1,)))
        begin(now, chunk)
        if chunk < chunks - 1:
            now = arrivals(now, now + GRACE, ((0,), (1,)))
    arrivals(now, math.inf, ((0,), (1,), (2,), (1, 2)))
    return plan


def apply_patch(u, diag, off, weight, orient, values, slopes):
    quad, ctrl = values.shape
    chunks = u.shape[3] // LANES
    points = quad * quad
    size = ctrl * ROWS
    forward, backward = plane_tables(values, slopes)
    scales = np.repeat(point_scales(values, slopes)[2][:, :, None], points, axis=2)
    vmem = pl.BlockSpec(memory_space=pltpu.VMEM)
    hbm = pl.BlockSpec(memory_space=pl.ANY)
    f32 = jnp.float32
    exchanged = [
        pltpu.VMEM((chunks, 2, 2, size, LANES), f32),
        pltpu.VMEM((chunks, 2, 2, ctrl, ctrl, LANES), f32),
    ]
    for planes in (INNER, ENDS, ALL):
        rows = len(span(planes, ctrl))
        exchanged.append(pltpu.VMEM((chunks, 2, 2, ctrl, rows, LANES), f32))
    for planes in (INNER, ENDS):
        rows = len(span(planes, ctrl))
        exchanged.append(pltpu.VMEM((chunks, 2, 2, 2, rows, LANES), f32))
    return pl.pallas_call(
        functools.partial(patch_kernel, values, slopes),
        out_shape=[pltpu.VMEM(u.shape, f32)] * 2,
        in_specs=[hbm] * 8,
        out_specs=[vmem, vmem],
        scratch_shapes=[
            pltpu.SMEM((3,), jnp.int32),
            pltpu.VMEM((chunks, ctrl, ctrl, ROWS, LANES), f32),
            pltpu.VMEM((7, quad, points), f32),
            pltpu.VMEM((7, quad, points), f32),
            pltpu.VMEM(forward.shape, jnp.bfloat16),
            pltpu.VMEM(backward.shape, f32),
            pltpu.VMEM((LANES, LANES), f32),
            pltpu.VMEM((7 * quad, points, LANES), f32),
            pltpu.VMEM((ctrl, 3 * points, LANES), f32),
            pltpu.VMEM((ctrl, 4 * points, LANES), f32),
            pltpu.VMEM((2 * size, 12 * points), jnp.bfloat16),
            pltpu.VMEM((chunks, 2, ctrl, size, LANES), f32),
            exchanged,
            exchanged,
            pltpu.VMEM((sent_rows(ctrl), LANES), f32),
            pltpu.SemaphoreType.DMA((chunks,)),
            pltpu.SemaphoreType.DMA((5,)),
            pltpu.SemaphoreType.DMA,
            pltpu.SemaphoreType.DMA((chunks, SLOTS)),
        ],
        compiler_params=pltpu.CompilerParams(collective_id=0, has_side_effects=True),
        name="apply_patch",
    )(
        orient, u, diag, off, weight,
        jnp.asarray(scales), jnp.asarray(forward), jnp.asarray(backward),
    )


def store_kernel(stiff, mass, stiff_out, mass_out, sem):
    copies = [
        pltpu.make_async_copy(stiff, stiff_out, sem.at[0]),
        pltpu.make_async_copy(mass, mass_out, sem.at[1]),
    ]
    for copy in copies:
        copy.start()
    for copy in copies:
        copy.wait()


def store_results(stiff, mass):
    vmem = pl.BlockSpec(memory_space=pltpu.VMEM)
    hbm = pl.BlockSpec(memory_space=pl.ANY)
    return pl.pallas_call(
        store_kernel,
        out_shape=[jax.ShapeDtypeStruct(stiff.shape, stiff.dtype)] * 2,
        in_specs=[vmem, vmem],
        out_specs=[hbm, hbm],
        scratch_shapes=[pltpu.SemaphoreType.DMA((2,))],
        name="store_results",
    )(*(pltpu.with_memory_space_constraint(x, pltpu.VMEM) for x in (stiff, mass)))


def per_device(control_values, metric_diag, metric_off, mass_weight, orient):
    values, slopes = spline_tables(mass_weight.shape[0] // 2)
    stiff, mass = apply_patch(
        control_values, metric_diag, metric_off, mass_weight, orient.reshape(3), values, slopes
    )
    return tuple(store_results(stiff, mass))


def solution(mesh):
    in_specs = (
        P("px", "py", "pz", None),
        P(None, "px", ("py", "pz")),
        P(None, "px", ("py", "pz")),
        P("px", ("py", "pz")),
        P("px", "py", "pz", None),
    )
    out_specs = (P("px", "py", "pz", None), P("px", "py", "pz", None))
    return jax.shard_map(
        per_device, mesh=mesh, in_specs=in_specs, out_specs=out_specs, check_vma=False
    )
```

```python
import functools
import heapq
import itertools
import math
from typing import NamedTuple

import jax
import jax.numpy as jnp
import numpy as np
from jax import lax
from jax.experimental import pallas as pl
from jax.experimental.pallas import tpu as pltpu
from jax.sharding import PartitionSpec as P

LANES = 128
ROWS = 8
AXES = ("px", "py", "pz")


def spline_tables(elements):
    knot_row = np.concatenate(
        [np.zeros(3), np.arange(elements + 1) * 1.0, np.full(3, float(elements))]
    )
    offsets = np.array([0.5 - 0.5 / math.sqrt(3.0), 0.5 + 0.5 / math.sqrt(3.0)])
    points = (np.arange(elements)[:, None] + offsets[None, :]).reshape(-1)
    intervals = np.repeat(np.arange(elements), 2) + 3
    current = np.zeros((points.size, knot_row.size - 1))
    current[np.arange(points.size), intervals] = 1.0
    previous = current
    for degree in range(1, 4):
        columns = knot_row.size - 1 - degree
        updated = np.zeros((points.size, columns))
        for i in range(columns):
            lower_gap = knot_row[i + degree] - knot_row[i]
            upper_gap = knot_row[i + degree + 1] - knot_row[i + 1]
            if lower_gap > 0:
                updated[:, i] += (points - knot_row[i]) / lower_gap * current[:, i]
            if upper_gap > 0:
                updated[:, i] += (knot_row[i + degree + 1] - points) / upper_gap * current[:, i + 1]
        previous = current
        current = updated
    slopes = np.zeros(current.shape)
    for i in range(current.shape[1]):
        lower_gap = knot_row[i + 3] - knot_row[i]
        upper_gap = knot_row[i + 4] - knot_row[i + 1]
        if lower_gap > 0:
            slopes[:, i] += 3.0 / lower_gap * previous[:, i]
        if upper_gap > 0:
            slopes[:, i] -= 3.0 / upper_gap * previous[:, i + 1]
    return (current.astype(np.float32), slopes.astype(np.float32))


def split(x):
    high = x.astype(jnp.bfloat16)
    return high, (x - high.astype(jnp.float32)).astype(jnp.bfloat16)


def split_table(table):
    high = table.astype(jnp.bfloat16)
    low = (table - high.astype(np.float32)).astype(jnp.bfloat16)
    return np.asarray(high), np.asarray(low)


def place(index, ctrl):
    return (0, *range(2, ctrl), 1)[index]


def plane_tables(values, slopes):
    quad, ctrl = values.shape
    wide = np.zeros((quad, ROWS), np.float64)
    tall = np.zeros((quad, ROWS), np.float64)
    wide[:, :ctrl] = values
    tall[:, :ctrl] = slopes
    fields = [np.kron(wide, wide), np.kron(tall, wide), np.kron(wide, tall)]
    forward = np.concatenate(fields, 0).astype(np.float32)
    high, low = split_table(forward)
    forward = np.concatenate([high, high, low], 1)
    backward = []
    size = ctrl * ROWS
    for flip_y in range(2):
        for flip_z in range(2):
            rows = np.full(size, -1)
            for j in range(ctrl):
                for k in range(ctrl):
                    jj = ctrl - 1 - j if flip_y else j
                    kk = ctrl - 1 - k if flip_z else k
                    rows[place(j, ctrl) * ROWS + k] = jj * ROWS + kk
            back = [np.where(rows[:, None] >= 0, f.T[rows], 0.0) for f in fields]
            none = np.zeros_like(back[0])
            stiff = np.concatenate([back[0], back[1], back[2], none], 1)
            mass = np.concatenate([none, none, none, back[0]], 1)
            backward.append(np.concatenate([stiff, mass], 0).astype(np.float32))
    return forward, np.stack(backward)


def point_scales(values, slopes):
    v = np.take_along_axis(values, np.abs(values).argmax(1)[:, None], 1)[:, 0]
    s = np.take_along_axis(slopes, np.abs(slopes).argmax(1)[:, None], 1)[:, 0]
    v, s = v.astype(np.float64), s.astype(np.float64)
    scales = np.stack([s * s, v * v, v * v, s * v, s * v, v * v, v * v])
    return v, s, scales.astype(np.float32)


def combine(weights, terms):
    total = None
    for weight, term in zip(weights, terms):
        term = term if weight == 1.0 else weight * term
        total = term if total is None else total + term
    return total


SPREAD = 28
FIRST = True
ENDS, INNER, ALL = slice(0, 2), slice(2, None), slice(None)


def span(planes, ctrl):
    return range(ctrl)[planes]


class Move(NamedTuple):
    axes: tuple
    x: slice | None
    y: slice | None
    after: tuple = ()

    def points(self, ctrl):
        sizes = [len(span(planes, ctrl)) for planes in (self.x, self.y) if planes is not None]
        return math.prod(sizes) * {(0,): ROWS, (1,): ctrl}.get(self.axes, 1)


CHAIN = (
    Move((0,), None, ENDS),
    Move((0,), None, INNER),
    Move((1,), INNER, None),
    Move((2,), INNER, INNER),
    Move((1,), ENDS, None, (0,)),
    Move((2,), ENDS, INNER, (1,)),
    Move((2,), ALL, ENDS, (2, 4)),
)
DIRECT = (
    Move((0,), None, ENDS),
    Move((0,), None, INNER),
    Move((1, 2), INNER, None),
    Move((1,), INNER, None),
    Move((2,), INNER, ALL),
    Move((1, 2), ENDS, None, (0,)),
    Move((1,), ENDS, None, (0,)),
    Move((2,), ENDS, ALL, (0, 1)),
)
MOVES = (CHAIN, CHAIN, CHAIN, DIRECT)


def sent_rows(ctrl):
    return sum(move.points(ctrl) * 2 ** len(move.axes) * 2 for moves in MOVES for move in moves)


class Exchange:
    def __init__(self, state, sends, bufs, tally, send_sem, recv_sem, nbrs):
        self.state, self.sends, self.bufs, self.tally = state, sends, bufs, tally
        self.send_sem, self.recv_sem, self.nbrs = send_sem, recv_sem, nbrs
        self.ctrl = state.shape[2]

    def parts(self, c, m):
        move, ctrl = MOVES[c][m], self.ctrl
        for f in range(2):
            for sides in itertools.product(range(2), repeat=len(move.axes)):
                if move.axes == (0,):
                    rows = self.block(move)
                    yield sides, (c, f, sides[0], rows), (c, *sides, f, rows)
                    continue
                for n, i in enumerate(span(move.x, ctrl)):
                    if move.axes == (1,):
                        rows = pl.ds(sides[0] * ROWS, ctrl)
                        yield sides, (c, f, i, rows), (c, *sides, f, i)
                    elif move.axes == (2,):
                        y = span(move.y, ctrl)
                        start = y[0] * ROWS + sides[0] * (ctrl - 1)
                        rows = pl.ds(start, len(y), stride=ROWS)
                        yield sides, (c, f, i, rows), (c, *sides, f, i)
                    else:
                        row = sides[0] * ROWS + sides[1] * (ctrl - 1)
                        yield sides, (c, f, i, pl.ds(row, 1)), (c, *sides, f, pl.ds(n, 1))

    def block(self, move):
        y = span(move.y, self.ctrl)
        return slice(y[0] * ROWS, (y[-1] + 1) * ROWS)

    def view(self, bufs, c, m, sides):
        move = MOVES[c][m]
        index = (c, *sides) if sides else (c,) + (ALL,) * len(move.axes)
        if move.axes == (0,):
            return bufs[0].at[index + (ALL, self.block(move))]
        x = span(move.x, self.ctrl)
        if len(move.axes) == 1:
            index += (ALL, slice(x[0], x[-1] + 1))
        return self.buffer(bufs, move).at[index]

    def buffer(self, bufs, move):
        if move.axes == (2,):
            return bufs[2 + (INNER, ENDS, ALL).index(move.y)]
        if move.axes == (1, 2):
            return bufs[5 + (INNER, ENDS).index(move.x)]
        return bufs[move.axes[0]]

    def start(self, c, m):
        move = MOVES[c][m]
        send = self.buffer(self.sends, move)
        for _, here, there in self.parts(c, m):
            send[there] = self.state[here]
        for sides in itertools.product(range(2), repeat=len(move.axes)):
            opposite = tuple(1 - side for side in sides)
            pltpu.make_async_remote_copy(
                src_ref=self.view(self.sends, c, m, sides),
                dst_ref=self.view(self.bufs, c, m, opposite),
                send_sem=self.send_sem,
                recv_sem=self.arrived(c, m),
                device_id={AXES[a]: self.nbrs[a][side] for a, side in zip(move.axes, sides)},
                device_id_type=pl.DeviceIdType.MESH,
            ).start()

    def finish(self, c, m):
        move = MOVES[c][m]
        landed = self.view(self.bufs, c, m, None)
        pltpu.make_async_copy(landed, landed, self.arrived(c, m)).wait()
        buf = self.buffer(self.bufs, move)
        for _, here, there in self.parts(c, m):
            self.state[here] = self.state[here] + buf[there]

    def arrived(self, c, m):
        return self.recv_sem.at[sum(len(moves) for moves in MOVES[:c]) + m]

    def drain(self):
        pltpu.make_async_copy(self.tally, self.tally, self.send_sem).wait()


def patch_kernel(
    values, slopes, orient_hbm, u_hbm, diag_hbm, off_hbm, weight_hbm, scale_hbm, fwd_hbm, bwd_hbm,
    stiff_out, mass_out,
    orient, ubuf, metric, fwd, bwd, square, pick, coef, fields, back, table, state, sends, bufs,
    tally, u_sem, load_sem, send_sem, recv_sem,
):
    quad, ctrl = values.shape
    chunks = ubuf.shape[0]
    points = quad * quad
    size = ctrl * ROWS

    measures = [
        pltpu.make_async_copy(diag_hbm, metric.at[0:3], load_sem.at[0]),
        pltpu.make_async_copy(off_hbm, metric.at[3:6], load_sem.at[0]),
        pltpu.make_async_copy(weight_hbm, metric.at[6], load_sem.at[0]),
        pltpu.make_async_copy(scale_hbm, metric.at[7:14], load_sem.at[0]),
    ]
    loads = [
        pltpu.make_async_copy(
            u_hbm.at[:, :, :, c * LANES : (c + 1) * LANES], ubuf.at[c, :, :, 0:ctrl], u_sem.at[c]
        )
        for c in range(chunks)
    ]
    forward_load = pltpu.make_async_copy(fwd_hbm, fwd, load_sem.at[1])
    backward_loads = [
        pltpu.make_async_copy(bwd_hbm, bwd, load_sem.at[2]),
        pltpu.make_async_copy(orient_hbm, orient, load_sem.at[3]),
    ]
    for load in loads[:1] + measures + [forward_load] + loads[1:] + backward_loads:
        load.start()

    nbrs = []
    for axis in AXES:
        count, me = lax.axis_size(axis), lax.axis_index(axis)
        nbrs.append((lax.rem(me + count - 1, count), lax.rem(me + 1, count)))
    barrier = pltpu.get_barrier_semaphore()
    peers = [
        {AXES[a]: nbrs[a][side] for a, side in zip(axes, sides)}
        for axes in sorted({move.axes for moves in MOVES for move in moves})
        for sides in itertools.product(range(2), repeat=len(axes))
    ]
    for peer in peers:
        pl.semaphore_signal(barrier, inc=1, device_id=peer, device_id_type=pl.DeviceIdType.MESH)

    square[...] = jnp.zeros_like(square)
    column = lax.broadcasted_iota(jnp.int32, pick.shape, 1) // LANES
    odd = lax.rem(lax.broadcasted_iota(jnp.int32, pick.shape, 0), 2)
    pick[...] = jnp.where(odd == column, 1.0, 0.0).astype(jnp.bfloat16)
    def flips(shape):
        return [jnp.full(shape, orient[d], jnp.int32) == 1 for d in range(3)]

    value_scale, slope_scale, _ = point_scales(values, slopes)

    def pairs_of(c):
        for i in range(0, ctrl, 2):
            yield c, [p for p in (i, i + 1) if p < ctrl]

    def expand(c, pair):
        none = jnp.zeros((ROWS * ROWS - size, LANES), jnp.float32)
        for p in pair:
            ubuf[c, p, :, ctrl:ROWS, :] = jnp.zeros((ctrl, ROWS - ctrl, LANES), jnp.float32)
        planes = [jnp.concatenate([ubuf[c, p].reshape(size, LANES), none], axis=0) for p in pair]
        high, low = split(jnp.concatenate(planes, axis=1))
        stacked = jnp.concatenate([high, low, high], axis=0)
        result = jnp.dot(fwd[...], stacked, preferred_element_type=jnp.float32)
        for n, p in enumerate(pair):
            fields[p] = result[:, n * LANES : (n + 1) * LANES]

    def weigh():
        @pl.loop(0, quad)
        def _(b):
            row = pl.multiple_of(b * ROWS, ROWS)
            part = [
                [fields[i, pl.ds(f * points + row, ROWS), :] for f in range(3)]
                for i in range(ctrl)
            ]
            acc = [[None] * ctrl for _ in range(4)]
            for q in range(quad):
                near = [i for i in range(ctrl) if values[q, i] != 0.0 or slopes[q, i] != 0.0]
                v = [float(values[q, i] / value_scale[q]) for i in near]
                s = [float(slopes[q, i] / slope_scale[q]) for i in near]
                g1 = combine(s, [part[i][0] for i in near])
                p = combine(v, [part[i][0] for i in near])
                g2 = combine(v, [part[i][1] for i in near])
                g3 = combine(v, [part[i][2] for i in near])
                d = [coef[t * quad + q, pl.ds(row, ROWS), :] for t in range(7)]
                flux = [
                    d[0] * g1 + d[3] * g2 + d[4] * g3,
                    d[3] * g1 + d[1] * g2 + d[5] * g3,
                    d[4] * g1 + d[5] * g2 + d[2] * g3,
                    d[6] * p,
                ]
                for f in range(4):
                    for n, i in enumerate(near):
                        weight = s[n] if f == 0 else v[n]
                        term = flux[f] if weight == 1.0 else weight * flux[f]
                        acc[f][i] = term if acc[f][i] is None else acc[f][i] + term
            for f in range(4):
                for i in range(ctrl):
                    back[i, pl.ds(f * points + row, ROWS), :] = acc[f][i]

    def select_table():
        for load in backward_loads:
            load.wait()
        _, flip_y, flip_z = flips((2 * size, 4 * points))
        high, low = split(
            jnp.where(flip_y, jnp.where(flip_z, bwd[3], bwd[2]), jnp.where(flip_z, bwd[1], bwd[0]))
        )
        columns = 4 * points
        table[:, 0:columns] = high
        table[:, columns : 2 * columns] = low
        table[:, 2 * columns : 3 * columns] = high

    def collect(c, later=None):
        flip_block = flips((2 * size, LANES))[0]
        jobs = [] if later is None else list(pairs_of(later))
        for i in range((ctrl + 1) // 2):
            if i < len(jobs):
                expand(*jobs[i])
            pair = [i, ctrl - 1 - i][: 1 if 2 * i == ctrl - 1 else 2]
            high, low = split(jnp.concatenate([back[p] for p in pair], axis=1))
            stacked = jnp.concatenate([high, high, low], axis=0)
            total = jnp.dot(table[...], stacked, preferred_element_type=jnp.float32)
            sums = [total[:, n * LANES : (n + 1) * LANES] for n in range(len(pair))]
            for p, own, other in zip(pair, sums, sums[::-1]):
                plane = own if len(pair) == 1 else jnp.where(flip_block, other, own)
                for f in range(2):
                    state[c, f, place(p, ctrl)] = plane[f * size : (f + 1) * size]

    pltpu.make_async_copy(metric, metric, load_sem.at[0]).wait()
    forward_load.wait()
    loads[0].wait()
    for t in range(7):
        square[t * quad : (t + 1) * quad, 0:points] = metric[t] * metric[7 + t]
    square[...] = square[...].T
    across = square[0:points]
    spread = SPREAD
    if FIRST:
        for job in pairs_of(0):
            expand(*job)
    for t in range(spread):
        coef[t] = jnp.broadcast_to(across[:, t : t + 1], (points, LANES))
    high, low = split(across)
    halves = [high.astype(jnp.float32), low.astype(jnp.float32)]
    lane = lax.broadcasted_iota(jnp.int32, across.shape, 1) // 2
    pairs = range(spread // 2, 7 * quad // 2)
    masked = [
        jnp.concatenate([jnp.where(lane == m, half, 0.0).astype(jnp.bfloat16) for m in pairs], 0)
        for half in halves
    ]
    spreads = jnp.dot(
        jnp.concatenate(masked, axis=1), pick[...], preferred_element_type=jnp.float32
    )
    for n, m in enumerate(pairs):
        for t in range(2):
            coef[2 * m + t] = spreads[n * points : (n + 1) * points, t * LANES : (t + 1) * LANES]
    if not FIRST:
        for job in pairs_of(0):
            expand(*job)

    exchange = Exchange(state, sends, bufs, tally, send_sem, recv_sem, nbrs)
    index = lax.broadcasted_iota(jnp.int32, (ROWS, LANES), 0)
    index = jnp.maximum(ctrl - 1 - index, 0)
    for step, c, m in exchange_plan(chunks, ctrl):
        if step == "weigh":
            weigh()
            if c == 0:
                select_table()
        if step == "collect":
            collect(c)
            if c == 0:
                pl.semaphore_wait(barrier, len(peers))
        if step == "expand":
            loads[c].wait()
            for job in pairs_of(c):
                expand(*job)
        if step == "both":
            loads[c + 1].wait()
            collect(c, c + 1)
        if step == "start":
            exchange.start(c, m)
        if step == "finish":
            exchange.finish(c, m)
        if step != "final":
            continue
        flip_x, flip_y, flip_z = flips((ROWS, LANES))
        lanes = slice(c * LANES, (c + 1) * LANES)
        for f, i, j in itertools.product(range(2), range(ctrl), range(ctrl)):
            x = [
                [
                    state[c, f, place(ii, ctrl), jj * ROWS : (jj + 1) * ROWS]
                    for jj in (place(j, ctrl), place(ctrl - 1 - j, ctrl))
                ]
                for ii in (i, ctrl - 1 - i)
            ]
            x = [jnp.where(flip_y, y[1], y[0]) for y in x]
            x = jnp.where(flip_x, x[1], x[0])
            other = jnp.take_along_axis(x, index, axis=0, mode="promise_in_bounds")
            (stiff_out, mass_out)[f][i, j, :, lanes] = jnp.where(flip_z, other, x)[0:ctrl]
    exchange.drain()


RATE = (0.022, 0.04, 0.04)
LATENCY = (2.1, 3.4, 6.0)
TIMES = {"weigh": 0.62, "collect": 0.38, "expand": 0.27, "both": 0.48, "start": 0.03, "finish": 0.03, "final": 0.05}
WINDOW = 0.8
MERGE = True
GRACE = -0.5


def exchange_plan(chunks, ctrl):
    free = [0.0, 0.0, 0.0]
    plan, ready, pending, begun = [], [], [], set()
    folded = [set() for _ in range(chunks)]
    work = []
    for chunk in range(chunks):
        if MERGE and 0 < chunk < chunks - 1:
            work += [("weigh", chunk), ("both", chunk)]
            continue
        work += [("weigh", chunk), ("collect", chunk)]
        work += [("expand", chunk + 1)] if chunk + 1 < chunks else []
    work.reverse()
    now = 0.0

    def step(name, chunk, m=None):
        nonlocal now
        plan.append((name, chunk, m))
        now += TIMES[name]

    def release(chunk, done):
        for m, move in enumerate(MOVES[chunk]):
            after = set(move.after)
            if (done in after if after else done is None) and folded[chunk] >= after:
                followers = sum(m in other.after for other in MOVES[chunk])
                ready.append((0 not in move.axes, -followers, len(move.after) == 0, chunk, m))
        ready.sort()

    def held(chunk, m):
        followed = any(m in other.after for other in MOVES[chunk])
        return not followed and MOVES[chunk][m].axes == (1,) and any(
            (c, n) not in begun
            for c in range(chunk)
            for n, move in enumerate(MOVES[c])
            if move.axes == (1,) and any(n in other.after for other in MOVES[c])
        )

    def foldable(chunk, m):
        after = set(MOVES[chunk][m].after)
        return all(
            (chunk, n) in begun
            for n, move in enumerate(MOVES[chunk])
            if n == m or 0 not in move.axes and (set(move.after) <= after or not move.after)
        )

    def issue():
        nonlocal now
        for item in list(ready):
            chunk, m = item[-2:]
            move = MOVES[chunk][m]
            if 0 in move.axes or not held(chunk, m) and max(free[a] for a in move.axes) <= now + WINDOW:
                ready.remove(item)
                begun.add((chunk, m))
                step("start", chunk, m)
                cost = move.points(ctrl) * 2 ** (len(move.axes) - 1)
                for a in move.axes:
                    free[a] = max(free[a], now) + cost * RATE[a]
                late = max(free[a] + LATENCY[a] for a in move.axes)
                heapq.heappush(pending, (late, chunk, m))

    while work or ready or pending:
        issue()
        able = sorted(p for p in pending if foldable(*p[1:]))
        near = [p for p in able if 2 not in MOVES[p[1]][p[2]].axes and p[0] <= now + GRACE]
        if work and not near:
            name, chunk = work.pop()
            step(name, chunk)
            if name in ("collect", "both"):
                release(chunk, None)
            continue
        if not able:
            now += WINDOW / 8
            continue
        late, chunk, m = near[0] if near else able[0]
        pending.remove((late, chunk, m))
        heapq.heapify(pending)
        now = max(now, late)
        step("finish", chunk, m)
        folded[chunk].add(m)
        release(chunk, m)
        if len(folded[chunk]) == len(MOVES[chunk]):
            step("final", chunk)
    return plan


def apply_patch(u, diag, off, weight, orient, values, slopes):
    quad, ctrl = values.shape
    chunks = u.shape[3] // LANES
    points = quad * quad
    size = ctrl * ROWS
    forward, backward = plane_tables(values, slopes)
    scales = np.repeat(point_scales(values, slopes)[2][:, :, None], points, axis=2)
    vmem = pl.BlockSpec(memory_space=pltpu.VMEM)
    hbm = pl.BlockSpec(memory_space=pl.ANY)
    f32 = jnp.float32
    exchanged = [
        pltpu.VMEM((chunks, 2, 2, size, LANES), f32),
        pltpu.VMEM((chunks, 2, 2, ctrl, ctrl, LANES), f32),
    ]
    for planes in (INNER, ENDS, ALL):
        rows = len(span(planes, ctrl))
        exchanged.append(pltpu.VMEM((chunks, 2, 2, ctrl, rows, LANES), f32))
    for planes in (INNER, ENDS):
        rows = len(span(planes, ctrl))
        exchanged.append(pltpu.VMEM((chunks, 2, 2, 2, rows, LANES), f32))
    return pl.pallas_call(
        functools.partial(patch_kernel, values, slopes),
        out_shape=[pltpu.VMEM(u.shape, f32)] * 2,
        in_specs=[hbm] * 8,
        out_specs=[vmem, vmem],
        scratch_shapes=[
            pltpu.SMEM((3,), jnp.int32),
            pltpu.VMEM((chunks, ctrl, ctrl, ROWS, LANES), f32),
            pltpu.VMEM((14, quad, points), f32),
            pltpu.VMEM(forward.shape, jnp.bfloat16),
            pltpu.VMEM(backward.shape, f32),
            pltpu.VMEM((LANES, LANES), f32),
            pltpu.VMEM((2 * LANES, 2 * LANES), jnp.bfloat16),
            pltpu.VMEM((7 * quad, points, LANES), f32),
            pltpu.VMEM((ctrl, 3 * points, LANES), f32),
            pltpu.VMEM((ctrl, 4 * points, LANES), f32),
            pltpu.VMEM((2 * size, 12 * points), jnp.bfloat16),
            pltpu.VMEM((chunks, 2, ctrl, size, LANES), f32),
            exchanged,
            exchanged,
            pltpu.VMEM((sent_rows(ctrl), LANES), f32),
            pltpu.SemaphoreType.DMA((chunks,)),
            pltpu.SemaphoreType.DMA((4,)),
            pltpu.SemaphoreType.DMA,
            pltpu.SemaphoreType.DMA((sum(len(moves) for moves in MOVES),)),
        ],
        compiler_params=pltpu.CompilerParams(collective_id=0, has_side_effects=True),
        name="apply_patch",
    )(
        orient, u, diag, off, weight,
        jnp.asarray(scales), jnp.asarray(forward), jnp.asarray(backward),
    )


def store_kernel(stiff, mass, stiff_out, mass_out, sem):
    copies = [
        pltpu.make_async_copy(stiff, stiff_out, sem.at[0]),
        pltpu.make_async_copy(mass, mass_out, sem.at[1]),
    ]
    for copy in copies:
        copy.start()
    for copy in copies:
        copy.wait()


def store_results(stiff, mass):
    vmem = pl.BlockSpec(memory_space=pltpu.VMEM)
    hbm = pl.BlockSpec(memory_space=pl.ANY)
    return pl.pallas_call(
        store_kernel,
        out_shape=[jax.ShapeDtypeStruct(stiff.shape, stiff.dtype)] * 2,
        in_specs=[vmem, vmem],
        out_specs=[hbm, hbm],
        scratch_shapes=[pltpu.SemaphoreType.DMA((2,))],
        name="store_results",
    )(*(pltpu.with_memory_space_constraint(x, pltpu.VMEM) for x in (stiff, mass)))


def per_device(control_values, metric_diag, metric_off, mass_weight, orient):
    values, slopes = spline_tables(mass_weight.shape[0] // 2)
    stiff, mass = apply_patch(
        control_values, metric_diag, metric_off, mass_weight, orient.reshape(3), values, slopes
    )
    return tuple(store_results(stiff, mass))


def solution(mesh):
    in_specs = (
        P("px", "py", "pz", None),
        P(None, "px", ("py", "pz")),
        P(None, "px", ("py", "pz")),
        P("px", ("py", "pz")),
        P("px", "py", "pz", None),
    )
    out_specs = (P("px", "py", "pz", None), P("px", "py", "pz", None))
    return jax.shard_map(
        per_device, mesh=mesh, in_specs=in_specs, out_specs=out_specs, check_vma=False
    )
```

```python
import functools
import heapq
import itertools
import math
from typing import NamedTuple

import jax
import jax.numpy as jnp
import numpy as np
from jax import lax
from jax.experimental import pallas as pl
from jax.experimental.pallas import tpu as pltpu
from jax.sharding import PartitionSpec as P

LANES = 128
ROWS = 8
AXES = ("px", "py", "pz")


def spline_tables(elements):
    knot_row = np.concatenate(
        [np.zeros(3), np.arange(elements + 1) * 1.0, np.full(3, float(elements))]
    )
    offsets = np.array([0.5 - 0.5 / math.sqrt(3.0), 0.5 + 0.5 / math.sqrt(3.0)])
    points = (np.arange(elements)[:, None] + offsets[None, :]).reshape(-1)
    intervals = np.repeat(np.arange(elements), 2) + 3
    current = np.zeros((points.size, knot_row.size - 1))
    current[np.arange(points.size), intervals] = 1.0
    previous = current
    for degree in range(1, 4):
        columns = knot_row.size - 1 - degree
        updated = np.zeros((points.size, columns))
        for i in range(columns):
            lower_gap = knot_row[i + degree] - knot_row[i]
            upper_gap = knot_row[i + degree + 1] - knot_row[i + 1]
            if lower_gap > 0:
                updated[:, i] += (points - knot_row[i]) / lower_gap * current[:, i]
            if upper_gap > 0:
                updated[:, i] += (knot_row[i + degree + 1] - points) / upper_gap * current[:, i + 1]
        previous = current
        current = updated
    slopes = np.zeros(current.shape)
    for i in range(current.shape[1]):
        lower_gap = knot_row[i + 3] - knot_row[i]
        upper_gap = knot_row[i + 4] - knot_row[i + 1]
        if lower_gap > 0:
            slopes[:, i] += 3.0 / lower_gap * previous[:, i]
        if upper_gap > 0:
            slopes[:, i] -= 3.0 / upper_gap * previous[:, i + 1]
    return (current.astype(np.float32), slopes.astype(np.float32))


def split(x):
    high = x.astype(jnp.bfloat16)
    return high, (x - high.astype(jnp.float32)).astype(jnp.bfloat16)


def split_table(table):
    high = table.astype(jnp.bfloat16)
    low = (table - high.astype(np.float32)).astype(jnp.bfloat16)
    return np.asarray(high), np.asarray(low)


def place(index, ctrl):
    return (0, *range(2, ctrl), 1)[index]


def plane_tables(values, slopes):
    quad, ctrl = values.shape
    wide = np.zeros((quad, ROWS), np.float64)
    tall = np.zeros((quad, ROWS), np.float64)
    wide[:, :ctrl] = values
    tall[:, :ctrl] = slopes
    fields = [np.kron(wide, wide), np.kron(tall, wide), np.kron(wide, tall)]
    forward = np.concatenate(fields, 0).astype(np.float32)
    high, low = split_table(forward)
    forward = np.concatenate([high, high, low], 1)
    backward = []
    size = ctrl * ROWS
    for flip_y in range(2):
        for flip_z in range(2):
            rows = np.full(size, -1)
            for j in range(ctrl):
                for k in range(ctrl):
                    jj = ctrl - 1 - j if flip_y else j
                    kk = ctrl - 1 - k if flip_z else k
                    rows[place(j, ctrl) * ROWS + k] = jj * ROWS + kk
            back = [np.where(rows[:, None] >= 0, f.T[rows], 0.0) for f in fields]
            none = np.zeros_like(back[0])
            stiff = np.concatenate([back[0], back[1], back[2], none], 1)
            mass = np.concatenate([none, none, none, back[0]], 1)
            backward.append(np.concatenate([stiff, mass], 0).astype(np.float32))
    return forward, np.stack(backward)


def point_scales(values, slopes):
    v = np.take_along_axis(values, np.abs(values).argmax(1)[:, None], 1)[:, 0]
    s = np.take_along_axis(slopes, np.abs(slopes).argmax(1)[:, None], 1)[:, 0]
    v, s = v.astype(np.float64), s.astype(np.float64)
    scales = np.stack([s * s, v * v, v * v, s * v, s * v, v * v, v * v])
    return v, s, scales.astype(np.float32)


def combine(weights, terms):
    total = None
    for weight, term in zip(weights, terms):
        term = term if weight == 1.0 else weight * term
        total = term if total is None else total + term
    return total


SPREAD = 28
ENDS, INNER, ALL = slice(0, 2), slice(2, None), slice(None)


def span(planes, ctrl):
    return range(ctrl)[planes]


class Move(NamedTuple):
    axes: tuple
    x: slice | None
    y: slice | None
    after: tuple = ()

    def key(self):
        return self.axes, str(self.y), str(self.x) if len(self.axes) == 2 else None

    def points(self, ctrl):
        sizes = [len(span(planes, ctrl)) for planes in (self.x, self.y) if planes is not None]
        return math.prod(sizes) * {(0,): ROWS, (1,): ctrl}.get(self.axes, 1)


CHAIN = (
    Move((0,), None, ENDS),
    Move((0,), None, INNER),
    Move((1,), INNER, None),
    Move((2,), INNER, INNER),
    Move((1,), ENDS, None, (0,)),
    Move((2,), ENDS, INNER, (1,)),
    Move((2,), ALL, ENDS, (2, 4)),
)
DIRECT = (
    Move((0,), None, ENDS),
    Move((0,), None, INNER),
    Move((1, 2), INNER, None),
    Move((1,), INNER, None),
    Move((2,), INNER, ALL),
    Move((1, 2), ENDS, None, (0,)),
    Move((1,), ENDS, None, (0,)),
    Move((2,), ENDS, ALL, (0, 1)),
)
MOVES = (CHAIN, CHAIN, CHAIN, DIRECT)


def group(c, m):
    return tuple(n for n, move in enumerate(MOVES[c]) if move.key() == MOVES[c][m].key())


def groups(c):
    return sorted({group(c, m) for m in range(len(MOVES[c]))})


def sent_rows(ctrl):
    return sum(move.points(ctrl) * 2 ** len(move.axes) * 2 for moves in MOVES for move in moves)


class Exchange:
    def __init__(self, state, sends, bufs, tally, send_sem, recv_sem, nbrs):
        self.state, self.sends, self.bufs, self.tally = state, sends, bufs, tally
        self.send_sem, self.recv_sem, self.nbrs = send_sem, recv_sem, nbrs
        self.ctrl = state.shape[2]
        count, me = lax.axis_size(AXES[2]), lax.axis_index(AXES[2])
        self.far = jnp.where(me == count - 1, 1, 0)

    def parts(self, c, m):
        move, ctrl = MOVES[c][m], self.ctrl
        for f in range(2):
            for sides in itertools.product(range(2), repeat=len(move.axes)):
                if move.axes == (0,):
                    rows = self.block(move)
                    yield sides, (c, f, sides[0], rows), (c, *sides, f, rows)
                    continue
                for n, i in enumerate(span(move.x, ctrl)):
                    if move.axes == (1,):
                        rows = pl.ds(sides[0] * ROWS, ctrl)
                        yield sides, (c, f, i, rows), (c, *sides, f, i)
                    elif move.axes == (2,):
                        y = span(move.y, ctrl)
                        start = y[0] * ROWS + sides[0] * (ctrl - 1)
                        rows = pl.ds(start, len(y), stride=ROWS)
                        yield sides, (c, f, i, rows), (c, *sides, f, i)
                    else:
                        row = sides[0] * ROWS + sides[1] * (ctrl - 1)
                        yield sides, (c, f, i, pl.ds(row, 1)), (c, *sides, f, pl.ds(n, 1))

    def block(self, move):
        y = span(move.y, self.ctrl)
        return slice(y[0] * ROWS, (y[-1] + 1) * ROWS)

    def view(self, bufs, c, m, sides):
        move = MOVES[c][m]
        index = (c, *sides) if sides else (c,) + (ALL,) * len(move.axes)
        if move.axes == (0,):
            return bufs[0].at[index + (ALL, self.block(move))]
        x = span(move.x, self.ctrl)
        if len(move.axes) == 1:
            whole = sides is None and len(group(c, m)) > 1
            index += (ALL, ALL if whole else slice(x[0], x[-1] + 1))
        return self.buffer(bufs, move).at[index]

    def buffer(self, bufs, move):
        if move.axes == (2,):
            return bufs[2 + (INNER, ENDS, ALL).index(move.y)]
        if move.axes == (1, 2):
            return bufs[5 + (INNER, ENDS).index(move.x)]
        return bufs[move.axes[0]]

    def start(self, c, m):
        move = MOVES[c][m]
        send = self.buffer(self.sends, move)
        for _, here, there in self.parts(c, m):
            send[there] = self.state[here]
        for sides in itertools.product(range(2), repeat=len(move.axes)):
            targets = {AXES[a]: self.nbrs[a][side] for a, side in zip(move.axes, sides)}
            if 2 in move.axes:
                far = self.far
                *others, side = sides
                sides = (*others, far if side == 0 else 1 - far)
                before, behind = self.nbrs[2]
                targets[AXES[2]] = before + (behind - before) * sides[-1]
            opposite = tuple(1 - side for side in sides)
            pltpu.make_async_remote_copy(
                src_ref=self.view(self.sends, c, m, sides),
                dst_ref=self.view(self.bufs, c, m, opposite),
                send_sem=self.send_sem,
                recv_sem=self.arrived(c, m),
                device_id=targets,
                device_id_type=pl.DeviceIdType.MESH,
            ).start()

    def finish(self, c, m):
        move = MOVES[c][m]
        landed = self.view(self.bufs, c, m, None)
        pltpu.make_async_copy(landed, landed, self.arrived(c, m)).wait()
        buf = self.buffer(self.bufs, move)
        for n in group(c, m):
            for _, here, there in self.parts(c, n):
                self.state[here] = self.state[here] + buf[there]

    def arrived(self, c, m):
        before = sum(len(groups(chunk)) for chunk in range(c))
        return self.recv_sem.at[before + groups(c).index(group(c, m))]

    def drain(self):
        pltpu.make_async_copy(self.tally, self.tally, self.send_sem).wait()


def patch_kernel(
    values, slopes, orient_hbm, u_hbm, diag_hbm, off_hbm, weight_hbm, scale_hbm, fwd_hbm, bwd_hbm,
    stiff_out, mass_out,
    orient, ubuf, metric, fwd, bwd, square, pick, coef, fields, back, table, state, sends, bufs,
    tally, u_sem, load_sem, send_sem, recv_sem,
):
    quad, ctrl = values.shape
    chunks = ubuf.shape[0]
    points = quad * quad
    size = ctrl * ROWS

    measures = [
        pltpu.make_async_copy(diag_hbm, metric.at[0:3], load_sem.at[0]),
        pltpu.make_async_copy(off_hbm, metric.at[3:6], load_sem.at[0]),
        pltpu.make_async_copy(weight_hbm, metric.at[6], load_sem.at[0]),
        pltpu.make_async_copy(scale_hbm, metric.at[7:14], load_sem.at[0]),
    ]
    loads = [
        pltpu.make_async_copy(
            u_hbm.at[:, :, :, c * LANES : (c + 1) * LANES], ubuf.at[c, :, :, 0:ctrl], u_sem.at[c]
        )
        for c in range(chunks)
    ]
    forward_load = pltpu.make_async_copy(fwd_hbm, fwd, load_sem.at[1])
    backward_loads = [
        pltpu.make_async_copy(bwd_hbm, bwd, load_sem.at[2]),
        pltpu.make_async_copy(orient_hbm, orient, load_sem.at[3]),
    ]
    for load in loads[:1] + measures + [forward_load] + loads[1:] + backward_loads:
        load.start()

    nbrs = []
    for axis in AXES:
        count, me = lax.axis_size(axis), lax.axis_index(axis)
        nbrs.append((lax.rem(me + count - 1, count), lax.rem(me + 1, count)))
    barrier = pltpu.get_barrier_semaphore()
    peers = [
        {AXES[a]: nbrs[a][side] for a, side in zip(axes, sides)}
        for axes in sorted({move.axes for moves in MOVES for move in moves})
        for sides in itertools.product(range(2), repeat=len(axes))
    ]
    for peer in peers:
        pl.semaphore_signal(barrier, inc=1, device_id=peer, device_id_type=pl.DeviceIdType.MESH)

    square[...] = jnp.zeros_like(square)
    column = lax.broadcasted_iota(jnp.int32, pick.shape, 1) // LANES
    odd = lax.rem(lax.broadcasted_iota(jnp.int32, pick.shape, 0), 2)
    pick[...] = jnp.where(odd == column, 1.0, 0.0).astype(jnp.bfloat16)
    def flips(shape):
        return [jnp.full(shape, orient[d], jnp.int32) == 1 for d in range(3)]

    value_scale, slope_scale, _ = point_scales(values, slopes)

    def pairs_of(c):
        for i in range(0, ctrl, 2):
            yield c, [p for p in (i, i + 1) if p < ctrl]

    def expand(c, pair):
        none = jnp.zeros((ROWS * ROWS - size, LANES), jnp.float32)
        for p in pair:
            ubuf[c, p, :, ctrl:ROWS, :] = jnp.zeros((ctrl, ROWS - ctrl, LANES), jnp.float32)
        planes = [jnp.concatenate([ubuf[c, p].reshape(size, LANES), none], axis=0) for p in pair]
        high, low = split(jnp.concatenate(planes, axis=1))
        stacked = jnp.concatenate([high, low, high], axis=0)
        result = jnp.dot(fwd[...], stacked, preferred_element_type=jnp.float32)
        for n, p in enumerate(pair):
            fields[p] = result[:, n * LANES : (n + 1) * LANES]

    def weigh():
        @pl.loop(0, quad)
        def _(b):
            row = pl.multiple_of(b * ROWS, ROWS)
            part = [
                [fields[i, pl.ds(f * points + row, ROWS), :] for f in range(3)]
                for i in range(ctrl)
            ]
            acc = [[None] * ctrl for _ in range(4)]
            for q in range(quad):
                near = [i for i in range(ctrl) if values[q, i] != 0.0 or slopes[q, i] != 0.0]
                v = [float(values[q, i] / value_scale[q]) for i in near]
                s = [float(slopes[q, i] / slope_scale[q]) for i in near]
                g1 = combine(s, [part[i][0] for i in near])
                p = combine(v, [part[i][0] for i in near])
                g2 = combine(v, [part[i][1] for i in near])
                g3 = combine(v, [part[i][2] for i in near])
                d = [coef[t * quad + q, pl.ds(row, ROWS), :] for t in range(7)]
                flux = [
                    d[0] * g1 + d[3] * g2 + d[4] * g3,
                    d[3] * g1 + d[1] * g2 + d[5] * g3,
                    d[4] * g1 + d[5] * g2 + d[2] * g3,
                    d[6] * p,
                ]
                for f in range(4):
                    for n, i in enumerate(near):
                        weight = s[n] if f == 0 else v[n]
                        term = flux[f] if weight == 1.0 else weight * flux[f]
                        acc[f][i] = term if acc[f][i] is None else acc[f][i] + term
            for f in range(4):
                for i in range(ctrl):
                    back[i, pl.ds(f * points + row, ROWS), :] = acc[f][i]

    def select_table():
        for load in backward_loads:
            load.wait()
        _, flip_y, flip_z = flips((2 * size, 4 * points))
        high, low = split(
            jnp.where(flip_y, jnp.where(flip_z, bwd[3], bwd[2]), jnp.where(flip_z, bwd[1], bwd[0]))
        )
        columns = 4 * points
        table[:, 0:columns] = high
        table[:, columns : 2 * columns] = low
        table[:, 2 * columns : 3 * columns] = high

    def collect(c, later=None):
        flip_block = flips((2 * size, LANES))[0]
        jobs = [] if later is None else list(pairs_of(later))
        for i in range((ctrl + 1) // 2):
            if i < len(jobs):
                expand(*jobs[i])
            pair = [i, ctrl - 1 - i][: 1 if 2 * i == ctrl - 1 else 2]
            high, low = split(jnp.concatenate([back[p] for p in pair], axis=1))
            stacked = jnp.concatenate([high, high, low], axis=0)
            total = jnp.dot(table[...], stacked, preferred_element_type=jnp.float32)
            sums = [total[:, n * LANES : (n + 1) * LANES] for n in range(len(pair))]
            for p, own, other in zip(pair, sums, sums[::-1]):
                plane = own if len(pair) == 1 else jnp.where(flip_block, other, own)
                for f in range(2):
                    state[c, f, place(p, ctrl)] = plane[f * size : (f + 1) * size]

    pltpu.make_async_copy(metric, metric, load_sem.at[0]).wait()
    forward_load.wait()
    loads[0].wait()
    for t in range(7):
        square[t * quad : (t + 1) * quad, 0:points] = metric[t] * metric[7 + t]
    square[...] = square[...].T
    across = square[0:points]
    for t in range(SPREAD):
        coef[t] = jnp.broadcast_to(across[:, t : t + 1], (points, LANES))
    high, low = split(across)
    halves = [high.astype(jnp.float32), low.astype(jnp.float32)]
    lane = lax.broadcasted_iota(jnp.int32, across.shape, 1) // 2
    pairs = range(SPREAD // 2, 7 * quad // 2)
    masked = [
        jnp.concatenate([jnp.where(lane == m, half, 0.0).astype(jnp.bfloat16) for m in pairs], 0)
        for half in halves
    ]
    spreads = jnp.dot(
        jnp.concatenate(masked, axis=1), pick[...], preferred_element_type=jnp.float32
    )
    for n, m in enumerate(pairs):
        for t in range(2):
            coef[2 * m + t] = spreads[n * points : (n + 1) * points, t * LANES : (t + 1) * LANES]
    for job in pairs_of(0):
        expand(*job)

    exchange = Exchange(state, sends, bufs, tally, send_sem, recv_sem, nbrs)
    index = lax.broadcasted_iota(jnp.int32, (ROWS, LANES), 0)
    index = jnp.maximum(ctrl - 1 - index, 0)
    for step, c, m in exchange_plan(chunks, ctrl):
        if step == "weigh":
            weigh()
            if c == 0:
                select_table()
        if step == "collect":
            collect(c)
            if c == 0:
                pl.semaphore_wait(barrier, len(peers))
        if step == "expand":
            loads[c].wait()
            for job in pairs_of(c):
                expand(*job)
        if step == "both":
            loads[c + 1].wait()
            collect(c, c + 1)
        if step == "start":
            exchange.start(c, m)
        if step == "finish":
            exchange.finish(c, m)
        if step != "final":
            continue
        flip_x, flip_y, flip_z = flips((ROWS, LANES))
        lanes = slice(c * LANES, (c + 1) * LANES)
        for f, i, j in itertools.product(range(2), range(ctrl), range(ctrl)):
            x = [
                [
                    state[c, f, place(ii, ctrl), jj * ROWS : (jj + 1) * ROWS]
                    for jj in (place(j, ctrl), place(ctrl - 1 - j, ctrl))
                ]
                for ii in (i, ctrl - 1 - i)
            ]
            x = [jnp.where(flip_y, y[1], y[0]) for y in x]
            x = jnp.where(flip_x, x[1], x[0])
            other = jnp.take_along_axis(x, index, axis=0, mode="promise_in_bounds")
            (stiff_out, mass_out)[f][i, j, :, lanes] = jnp.where(flip_z, other, x)[0:ctrl]
    exchange.drain()


RATE = (0.022, 0.04, 0.04)
LATENCY = (2.1, 3.4, 6.0)
TIMES = {"weigh": 0.62, "collect": 0.38, "expand": 0.27, "both": 0.48, "start": 0.03, "finish": 0.03, "final": 0.05}
WINDOW = 0.8
TAIL = 3.0
GRACE = -0.5


def exchange_plan(chunks, ctrl):
    free = [0.0, 0.0, 0.0]
    plan, ready, pending, begun, arrival = [], [], [], set(), {}
    folded = [set() for _ in range(chunks)]
    work = []
    for chunk in range(chunks):
        if 0 < chunk < chunks - 1:
            work += [("weigh", chunk), ("both", chunk)]
            continue
        work += [("weigh", chunk), ("collect", chunk)]
        work += [("expand", chunk + 1)] if chunk + 1 < chunks else []
    work.reverse()
    now = 0.0

    def step(name, chunk, m=None):
        nonlocal now
        plan.append((name, chunk, m))
        now += TIMES[name]

    def release(chunk, done):
        for m, move in enumerate(MOVES[chunk]):
            after = set(move.after)
            if (after & done if after else not done) and folded[chunk] >= after:
                followers = sum(m in other.after for other in MOVES[chunk])
                ready.append((0 not in move.axes, -followers, len(move.after) == 0, chunk, m))
        ready.sort()

    def held(chunk, m):
        followed = any(m in other.after for other in MOVES[chunk])
        return not followed and 1 in MOVES[chunk][m].axes and any(
            (c, n) not in begun
            for c in range(chunk)
            for n, move in enumerate(MOVES[c])
            if move.axes == (1,) and any(n in other.after for other in MOVES[c])
        )

    def foldable(chunk, m):
        after = set(MOVES[chunk][m].after)
        return all(
            (chunk, n) in begun
            for n, move in enumerate(MOVES[chunk])
            if n == m or 0 not in move.axes and (set(move.after) <= after or not move.after)
        )

    def issue():
        nonlocal now
        for item in list(ready):
            chunk, m = item[-2:]
            move = MOVES[chunk][m]
            if 0 in move.axes or not held(chunk, m) and max(free[a] for a in move.axes) <= now + (WINDOW if work else TAIL):
                ready.remove(item)
                begun.add((chunk, m))
                step("start", chunk, m)
                cost = move.points(ctrl) * 2 ** (len(move.axes) - 1)
                for a in move.axes:
                    free[a] = max(free[a], now) + cost * RATE[a]
                late = max(free[a] + LATENCY[a] for a in move.axes)
                arrival[chunk, m] = late
                members = group(chunk, m)
                if all((chunk, n) in begun for n in members):
                    late = max(arrival[chunk, n] for n in members)
                    heapq.heappush(pending, (late, chunk, members[-1]))

    while work or ready or pending:
        issue()
        able = sorted(
            p for p in pending if all(foldable(p[1], n) for n in group(p[1], p[2]))
        )
        near = [p for p in able if 2 not in MOVES[p[1]][p[2]].axes and p[0] <= now + GRACE]
        if work and not near:
            name, chunk = work.pop()
            step(name, chunk)
            if name in ("collect", "both"):
                release(chunk, set())
            continue
        if not able:
            now += WINDOW / 8
            continue
        late, chunk, m = near[0] if near else able[0]
        pending.remove((late, chunk, m))
        heapq.heapify(pending)
        now = max(now, late)
        step("finish", chunk, m)
        folded[chunk].update(group(chunk, m))
        release(chunk, set(group(chunk, m)))
        if len(folded[chunk]) == len(MOVES[chunk]):
            step("final", chunk)
    return plan


def apply_patch(u, diag, off, weight, orient, values, slopes):
    quad, ctrl = values.shape
    chunks = u.shape[3] // LANES
    points = quad * quad
    size = ctrl * ROWS
    forward, backward = plane_tables(values, slopes)
    scales = np.repeat(point_scales(values, slopes)[2][:, :, None], points, axis=2)
    vmem = pl.BlockSpec(memory_space=pltpu.VMEM)
    hbm = pl.BlockSpec(memory_space=pl.ANY)
    f32 = jnp.float32
    exchanged = [
        pltpu.VMEM((chunks, 2, 2, size, LANES), f32),
        pltpu.VMEM((chunks, 2, 2, ctrl, ctrl, LANES), f32),
    ]
    for planes in (INNER, ENDS, ALL):
        rows = len(span(planes, ctrl))
        exchanged.append(pltpu.VMEM((chunks, 2, 2, ctrl, rows, LANES), f32))
    for planes in (INNER, ENDS):
        rows = len(span(planes, ctrl))
        exchanged.append(pltpu.VMEM((chunks, 2, 2, 2, rows, LANES), f32))
    return pl.pallas_call(
        functools.partial(patch_kernel, values, slopes),
        out_shape=[pltpu.VMEM(u.shape, f32)] * 2,
        in_specs=[hbm] * 8,
        out_specs=[vmem, vmem],
        scratch_shapes=[
            pltpu.SMEM((3,), jnp.int32),
            pltpu.VMEM((chunks, ctrl, ctrl, ROWS, LANES), f32),
            pltpu.VMEM((14, quad, points), f32),
            pltpu.VMEM(forward.shape, jnp.bfloat16),
            pltpu.VMEM(backward.shape, f32),
            pltpu.VMEM((LANES, LANES), f32),
            pltpu.VMEM((2 * LANES, 2 * LANES), jnp.bfloat16),
            pltpu.VMEM((7 * quad, points, LANES), f32),
            pltpu.VMEM((ctrl, 3 * points, LANES), f32),
            pltpu.VMEM((ctrl, 4 * points, LANES), f32),
            pltpu.VMEM((2 * size, 12 * points), jnp.bfloat16),
            pltpu.VMEM((chunks, 2, ctrl, size, LANES), f32),
            exchanged,
            exchanged,
            pltpu.VMEM((sent_rows(ctrl), LANES), f32),
            pltpu.SemaphoreType.DMA((chunks,)),
            pltpu.SemaphoreType.DMA((4,)),
            pltpu.SemaphoreType.DMA,
            pltpu.SemaphoreType.DMA((sum(len(groups(c)) for c in range(chunks)),)),
        ],
        compiler_params=pltpu.CompilerParams(collective_id=0, has_side_effects=True),
        name="apply_patch",
    )(
        orient, u, diag, off, weight,
        jnp.asarray(scales), jnp.asarray(forward), jnp.asarray(backward),
    )


def store_kernel(stiff, mass, stiff_out, mass_out, sem):
    copies = [
        pltpu.make_async_copy(stiff, stiff_out, sem.at[0]),
        pltpu.make_async_copy(mass, mass_out, sem.at[1]),
    ]
    for copy in copies:
        copy.start()
    for copy in copies:
        copy.wait()


def store_results(stiff, mass):
    vmem = pl.BlockSpec(memory_space=pltpu.VMEM)
    hbm = pl.BlockSpec(memory_space=pl.ANY)
    return pl.pallas_call(
        store_kernel,
        out_shape=[jax.ShapeDtypeStruct(stiff.shape, stiff.dtype)] * 2,
        in_specs=[vmem, vmem],
        out_specs=[hbm, hbm],
        scratch_shapes=[pltpu.SemaphoreType.DMA((2,))],
        name="store_results",
    )(*(pltpu.with_memory_space_constraint(x, pltpu.VMEM) for x in (stiff, mass)))


def per_device(control_values, metric_diag, metric_off, mass_weight, orient):
    values, slopes = spline_tables(mass_weight.shape[0] // 2)
    stiff, mass = apply_patch(
        control_values, metric_diag, metric_off, mass_weight, orient.reshape(3), values, slopes
    )
    return tuple(store_results(stiff, mass))


def solution(mesh):
    in_specs = (
        P("px", "py", "pz", None),
        P(None, "px", ("py", "pz")),
        P(None, "px", ("py", "pz")),
        P("px", ("py", "pz")),
        P("px", "py", "pz", None),
    )
    out_specs = (P("px", "py", "pz", None), P("px", "py", "pz", None))
    return jax.shard_map(
        per_device, mesh=mesh, in_specs=in_specs, out_specs=out_specs, check_vma=False
    )
```

```python
import functools
import heapq
import itertools
import math
from typing import NamedTuple

import jax
import jax.numpy as jnp
import numpy as np
from jax import lax
from jax.experimental import pallas as pl
from jax.experimental.pallas import tpu as pltpu
from jax.sharding import PartitionSpec as P

LANES = 128
ROWS = 8
AXES = ("px", "py", "pz")


def spline_tables(elements):
    knot_row = np.concatenate(
        [np.zeros(3), np.arange(elements + 1) * 1.0, np.full(3, float(elements))]
    )
    offsets = np.array([0.5 - 0.5 / math.sqrt(3.0), 0.5 + 0.5 / math.sqrt(3.0)])
    points = (np.arange(elements)[:, None] + offsets[None, :]).reshape(-1)
    intervals = np.repeat(np.arange(elements), 2) + 3
    current = np.zeros((points.size, knot_row.size - 1))
    current[np.arange(points.size), intervals] = 1.0
    previous = current
    for degree in range(1, 4):
        columns = knot_row.size - 1 - degree
        updated = np.zeros((points.size, columns))
        for i in range(columns):
            lower_gap = knot_row[i + degree] - knot_row[i]
            upper_gap = knot_row[i + degree + 1] - knot_row[i + 1]
            if lower_gap > 0:
                updated[:, i] += (points - knot_row[i]) / lower_gap * current[:, i]
            if upper_gap > 0:
                updated[:, i] += (knot_row[i + degree + 1] - points) / upper_gap * current[:, i + 1]
        previous = current
        current = updated
    slopes = np.zeros(current.shape)
    for i in range(current.shape[1]):
        lower_gap = knot_row[i + 3] - knot_row[i]
        upper_gap = knot_row[i + 4] - knot_row[i + 1]
        if lower_gap > 0:
            slopes[:, i] += 3.0 / lower_gap * previous[:, i]
        if upper_gap > 0:
            slopes[:, i] -= 3.0 / upper_gap * previous[:, i + 1]
    return (current.astype(np.float32), slopes.astype(np.float32))


def split(x):
    high = x.astype(jnp.bfloat16)
    return high, (x - high.astype(jnp.float32)).astype(jnp.bfloat16)


def split_table(table):
    high = table.astype(jnp.bfloat16)
    low = (table - high.astype(np.float32)).astype(jnp.bfloat16)
    return np.asarray(high), np.asarray(low)


def place(index, ctrl):
    return (0, *range(2, ctrl), 1)[index]


def plane_tables(values, slopes):
    quad, ctrl = values.shape
    wide = np.zeros((quad, ROWS), np.float64)
    tall = np.zeros((quad, ROWS), np.float64)
    wide[:, :ctrl] = values
    tall[:, :ctrl] = slopes
    fields = [np.kron(wide, wide), np.kron(tall, wide), np.kron(wide, tall)]
    forward = np.concatenate(fields, 0).astype(np.float32)
    high, low = split_table(forward)
    forward = np.concatenate([high, high, low], 1)
    backward = []
    size = ctrl * ROWS
    for flip_y in range(2):
        for flip_z in range(2):
            rows = np.full(size, -1)
            for j in range(ctrl):
                for k in range(ctrl):
                    jj = ctrl - 1 - j if flip_y else j
                    kk = ctrl - 1 - k if flip_z else k
                    rows[place(j, ctrl) * ROWS + k] = jj * ROWS + kk
            back = [np.where(rows[:, None] >= 0, f.T[rows], 0.0) for f in fields]
            none = np.zeros_like(back[0])
            stiff = np.concatenate([back[0], back[1], back[2], none], 1)
            mass = np.concatenate([none, none, none, back[0]], 1)
            backward.append(np.concatenate([stiff, mass], 0).astype(np.float32))
    return forward, np.stack(backward)


def point_scales(values, slopes):
    v = np.take_along_axis(values, np.abs(values).argmax(1)[:, None], 1)[:, 0]
    s = np.take_along_axis(slopes, np.abs(slopes).argmax(1)[:, None], 1)[:, 0]
    v, s = v.astype(np.float64), s.astype(np.float64)
    scales = np.stack([s * s, v * v, v * v, s * v, s * v, v * v, v * v])
    return v, s, scales.astype(np.float32)


def combine(weights, terms):
    total = None
    for weight, term in zip(weights, terms):
        term = term if weight == 1.0 else weight * term
        total = term if total is None else total + term
    return total


SPREAD = 28
ENDS, INNER, ALL = slice(0, 2), slice(2, None), slice(None)


def span(planes, ctrl):
    return range(ctrl)[planes]


class Move(NamedTuple):
    axes: tuple
    x: slice | None
    y: slice | None
    after: tuple = ()

    def key(self):
        return self.axes, str(self.y), str(self.x) if len(self.axes) == 2 else None

    def points(self, ctrl):
        sizes = [len(span(planes, ctrl)) for planes in (self.x, self.y) if planes is not None]
        return math.prod(sizes) * {(0,): ROWS, (1,): ctrl}.get(self.axes, 1)


CHAIN = (
    Move((0,), None, ENDS),
    Move((0,), None, INNER),
    Move((1,), INNER, None),
    Move((2,), INNER, INNER),
    Move((1,), ENDS, None, (0,)),
    Move((2,), ENDS, INNER, (1,)),
    Move((2,), ALL, ENDS, (2, 4)),
)
DIRECT = (
    Move((0,), None, ENDS),
    Move((0,), None, INNER),
    Move((1, 2), INNER, None),
    Move((1,), INNER, None),
    Move((2,), INNER, ALL),
    Move((1, 2), ENDS, None, (0,)),
    Move((1,), ENDS, None, (0,)),
    Move((2,), ENDS, ALL, (0, 1)),
)
MOVES = (CHAIN, CHAIN, CHAIN, DIRECT)


def group(c, m):
    return tuple(n for n, move in enumerate(MOVES[c]) if move.key() == MOVES[c][m].key())


def groups(c):
    return sorted({group(c, m) for m in range(len(MOVES[c]))})


def sent_rows(ctrl):
    return sum(move.points(ctrl) * 2 ** len(move.axes) * 2 for moves in MOVES for move in moves)


class Exchange:
    def __init__(self, state, sends, bufs, tally, send_sem, recv_sem, nbrs):
        self.state, self.sends, self.bufs, self.tally = state, sends, bufs, tally
        self.send_sem, self.recv_sem, self.nbrs = send_sem, recv_sem, nbrs
        self.ctrl = state.shape[2]
        count, me = lax.axis_size(AXES[2]), lax.axis_index(AXES[2])
        self.far = jnp.where(me == count - 1, 1, 0)

    def parts(self, c, m):
        move, ctrl = MOVES[c][m], self.ctrl
        for f in range(2):
            for sides in itertools.product(range(2), repeat=len(move.axes)):
                if move.axes == (0,):
                    rows = self.block(move)
                    yield sides, (c, f, sides[0], rows), (c, *sides, f, rows)
                    continue
                for n, i in enumerate(span(move.x, ctrl)):
                    if move.axes == (1,):
                        rows = pl.ds(sides[0] * ROWS, ctrl)
                        yield sides, (c, f, i, rows), (c, *sides, f, i)
                    elif move.axes == (2,):
                        y = span(move.y, ctrl)
                        start = y[0] * ROWS + sides[0] * (ctrl - 1)
                        rows = pl.ds(start, len(y), stride=ROWS)
                        yield sides, (c, f, i, rows), (c, *sides, f, i)
                    else:
                        row = sides[0] * ROWS + sides[1] * (ctrl - 1)
                        yield sides, (c, f, i, pl.ds(row, 1)), (c, *sides, f, pl.ds(n, 1))

    def block(self, move):
        y = span(move.y, self.ctrl)
        return slice(y[0] * ROWS, (y[-1] + 1) * ROWS)

    def view(self, bufs, c, m, sides):
        move = MOVES[c][m]
        index = (c, *sides) if sides else (c,) + (ALL,) * len(move.axes)
        if move.axes == (0,):
            return bufs[0].at[index + (ALL, self.block(move))]
        x = span(move.x, self.ctrl)
        if len(move.axes) == 1:
            whole = sides is None and len(group(c, m)) > 1
            index += (ALL, ALL if whole else slice(x[0], x[-1] + 1))
        return self.buffer(bufs, move).at[index]

    def buffer(self, bufs, move):
        if move.axes == (2,):
            return bufs[2 + (INNER, ENDS, ALL).index(move.y)]
        if move.axes == (1, 2):
            return bufs[5 + (INNER, ENDS).index(move.x)]
        return bufs[move.axes[0]]

    def start(self, c, m):
        move = MOVES[c][m]
        send = self.buffer(self.sends, move)
        for _, here, there in self.parts(c, m):
            send[there] = self.state[here]
        for sides in itertools.product(range(2), repeat=len(move.axes)):
            targets = {AXES[a]: self.nbrs[a][side] for a, side in zip(move.axes, sides)}
            if 2 in move.axes:
                far = self.far
                *others, side = sides
                sides = (*others, far if side == 0 else 1 - far)
                before, behind = self.nbrs[2]
                targets[AXES[2]] = before + (behind - before) * sides[-1]
            opposite = tuple(1 - side for side in sides)
            pltpu.make_async_remote_copy(
                src_ref=self.view(self.sends, c, m, sides),
                dst_ref=self.view(self.bufs, c, m, opposite),
                send_sem=self.send_sem,
                recv_sem=self.arrived(c, m),
                device_id=targets,
                device_id_type=pl.DeviceIdType.MESH,
            ).start()

    def finish(self, c, m):
        move = MOVES[c][m]
        landed = self.view(self.bufs, c, m, None)
        pltpu.make_async_copy(landed, landed, self.arrived(c, m)).wait()
        buf = self.buffer(self.bufs, move)
        for n in group(c, m):
            for _, here, there in self.parts(c, n):
                self.state[here] = self.state[here] + buf[there]

    def arrived(self, c, m):
        before = sum(len(groups(chunk)) for chunk in range(c))
        return self.recv_sem.at[before + groups(c).index(group(c, m))]

    def drain(self):
        pltpu.make_async_copy(self.tally, self.tally, self.send_sem).wait()


def patch_kernel(
    values, slopes, orient_hbm, u_hbm, diag_hbm, off_hbm, weight_hbm, scale_hbm, fwd_hbm, bwd_hbm,
    stiff_out, mass_out,
    orient, ubuf, metric, fwd, bwd, square, pick, coef, fields, back, table, state, sends, bufs,
    tally, u_sem, load_sem, send_sem, recv_sem,
):
    quad, ctrl = values.shape
    chunks = ubuf.shape[0]
    points = quad * quad
    size = ctrl * ROWS

    measures = [
        pltpu.make_async_copy(diag_hbm, metric.at[0:3], load_sem.at[0]),
        pltpu.make_async_copy(off_hbm, metric.at[3:6], load_sem.at[0]),
        pltpu.make_async_copy(weight_hbm, metric.at[6], load_sem.at[0]),
        pltpu.make_async_copy(scale_hbm, metric.at[7:14], load_sem.at[0]),
    ]
    loads = [
        pltpu.make_async_copy(
            u_hbm.at[:, :, :, c * LANES : (c + 1) * LANES], ubuf.at[c, :, :, 0:ctrl], u_sem.at[min(c, 1)]
        )
        for c in range(chunks)
    ]
    forward_load = pltpu.make_async_copy(fwd_hbm, fwd, load_sem.at[1])
    backward_loads = [
        pltpu.make_async_copy(bwd_hbm, bwd, load_sem.at[2]),
        pltpu.make_async_copy(orient_hbm, orient, load_sem.at[3]),
    ]
    for load in loads[:1] + measures + [forward_load] + loads[1:] + backward_loads:
        load.start()

    nbrs = []
    for axis in AXES:
        count, me = lax.axis_size(axis), lax.axis_index(axis)
        nbrs.append((lax.rem(me + count - 1, count), lax.rem(me + 1, count)))
    barrier = pltpu.get_barrier_semaphore()
    peers = [
        {AXES[a]: nbrs[a][side] for a, side in zip(axes, sides)}
        for axes in sorted({move.axes for moves in MOVES for move in moves})
        for sides in itertools.product(range(2), repeat=len(axes))
    ]
    for peer in peers:
        pl.semaphore_signal(barrier, inc=1, device_id=peer, device_id_type=pl.DeviceIdType.MESH)

    square[...] = jnp.zeros_like(square)
    column = lax.broadcasted_iota(jnp.int32, pick.shape, 1) // LANES
    odd = lax.rem(lax.broadcasted_iota(jnp.int32, pick.shape, 0), 2)
    pick[...] = jnp.where(odd == column, 1.0, 0.0).astype(jnp.bfloat16)
    def flips(shape):
        return [jnp.full(shape, orient[d], jnp.int32) == 1 for d in range(3)]

    value_scale, slope_scale, _ = point_scales(values, slopes)

    def pairs_of(c):
        for i in range(0, ctrl, 2):
            yield c, [p for p in (i, i + 1) if p < ctrl]

    def expand(c, pair):
        none = jnp.zeros((ROWS * ROWS - size, LANES), jnp.float32)
        for p in pair:
            ubuf[c, p, :, ctrl:ROWS, :] = jnp.zeros((ctrl, ROWS - ctrl, LANES), jnp.float32)
        planes = [jnp.concatenate([ubuf[c, p].reshape(size, LANES), none], axis=0) for p in pair]
        high, low = split(jnp.concatenate(planes, axis=1))
        stacked = jnp.concatenate([high, low, high], axis=0)
        result = jnp.dot(fwd[...], stacked, preferred_element_type=jnp.float32)
        for n, p in enumerate(pair):
            fields[p] = result[:, n * LANES : (n + 1) * LANES]

    def weigh():
        @pl.loop(0, quad)
        def _(b):
            row = pl.multiple_of(b * ROWS, ROWS)
            part = [
                [fields[i, pl.ds(f * points + row, ROWS), :] for f in range(3)]
                for i in range(ctrl)
            ]
            acc = [[None] * ctrl for _ in range(4)]
            for q in range(quad):
                near = [i for i in range(ctrl) if values[q, i] != 0.0 or slopes[q, i] != 0.0]
                v = [float(values[q, i] / value_scale[q]) for i in near]
                s = [float(slopes[q, i] / slope_scale[q]) for i in near]
                g1 = combine(s, [part[i][0] for i in near])
                p = combine(v, [part[i][0] for i in near])
                g2 = combine(v, [part[i][1] for i in near])
                g3 = combine(v, [part[i][2] for i in near])
                d = [coef[t * quad + q, pl.ds(row, ROWS), :] for t in range(7)]
                flux = [
                    d[0] * g1 + d[3] * g2 + d[4] * g3,
                    d[3] * g1 + d[1] * g2 + d[5] * g3,
                    d[4] * g1 + d[5] * g2 + d[2] * g3,
                    d[6] * p,
                ]
                for f in range(4):
                    for n, i in enumerate(near):
                        weight = s[n] if f == 0 else v[n]
                        term = flux[f] if weight == 1.0 else weight * flux[f]
                        acc[f][i] = term if acc[f][i] is None else acc[f][i] + term
            for f in range(4):
                for i in range(ctrl):
                    back[i, pl.ds(f * points + row, ROWS), :] = acc[f][i]

    def select_table():
        for load in backward_loads:
            load.wait()
        _, flip_y, flip_z = flips((2 * size, 4 * points))
        high, low = split(
            jnp.where(flip_y, jnp.where(flip_z, bwd[3], bwd[2]), jnp.where(flip_z, bwd[1], bwd[0]))
        )
        columns = 4 * points
        table[:, 0:columns] = high
        table[:, columns : 2 * columns] = low
        table[:, 2 * columns : 3 * columns] = high

    def collect(c, later=None):
        flip_block = flips((2 * size, LANES))[0]
        jobs = [] if later is None else list(pairs_of(later))
        for i in range((ctrl + 1) // 2):
            if i < len(jobs):
                expand(*jobs[i])
            pair = [i, ctrl - 1 - i][: 1 if 2 * i == ctrl - 1 else 2]
            high, low = split(jnp.concatenate([back[p] for p in pair], axis=1))
            stacked = jnp.concatenate([high, high, low], axis=0)
            total = jnp.dot(table[...], stacked, preferred_element_type=jnp.float32)
            sums = [total[:, n * LANES : (n + 1) * LANES] for n in range(len(pair))]
            for p, own, other in zip(pair, sums, sums[::-1]):
                plane = own if len(pair) == 1 else jnp.where(flip_block, other, own)
                for f in range(2):
                    state[c, f, place(p, ctrl)] = plane[f * size : (f + 1) * size]

    pltpu.make_async_copy(metric, metric, load_sem.at[0]).wait()
    forward_load.wait()
    loads[0].wait()
    for t in range(7):
        square[t * quad : (t + 1) * quad, 0:points] = metric[t] * metric[7 + t]
    square[...] = square[...].T
    across = square[0:points]
    for t in range(SPREAD):
        coef[t] = jnp.broadcast_to(across[:, t : t + 1], (points, LANES))
    high, low = split(across)
    halves = [high.astype(jnp.float32), low.astype(jnp.float32)]
    lane = lax.broadcasted_iota(jnp.int32, across.shape, 1) // 2
    pairs = range(SPREAD // 2, 7 * quad // 2)
    masked = [
        jnp.concatenate([jnp.where(lane == m, half, 0.0).astype(jnp.bfloat16) for m in pairs], 0)
        for half in halves
    ]
    spreads = jnp.dot(
        jnp.concatenate(masked, axis=1), pick[...], preferred_element_type=jnp.float32
    )
    for n, m in enumerate(pairs):
        for t in range(2):
            coef[2 * m + t] = spreads[n * points : (n + 1) * points, t * LANES : (t + 1) * LANES]
    for job in pairs_of(0):
        expand(*job)

    exchange = Exchange(state, sends, bufs, tally, send_sem, recv_sem, nbrs)
    index = lax.broadcasted_iota(jnp.int32, (ROWS, LANES), 0)
    index = jnp.maximum(ctrl - 1 - index, 0)
    for step, c, m in exchange_plan(chunks, ctrl):
        if step == "weigh":
            weigh()
            if c == 0:
                select_table()
        if step == "collect":
            collect(c)
            if c == 0:
                pl.semaphore_wait(barrier, len(peers))
        if step == "expand":
            if c == 1:
                rest = ubuf.at[1:chunks, :, :, 0:ctrl]
                pltpu.make_async_copy(rest, rest, u_sem.at[1]).wait()
            for job in pairs_of(c):
                expand(*job)
        if step == "both":
            collect(c, c + 1)
        if step == "start":
            exchange.start(c, m)
        if step == "finish":
            exchange.finish(c, m)
        if step != "final":
            continue
        flip_x, flip_y, flip_z = flips((ROWS, LANES))
        lanes = slice(c * LANES, (c + 1) * LANES)
        for f, i, j in itertools.product(range(2), range(ctrl), range(ctrl)):
            x = [
                [
                    state[c, f, place(ii, ctrl), jj * ROWS : (jj + 1) * ROWS]
                    for jj in (place(j, ctrl), place(ctrl - 1 - j, ctrl))
                ]
                for ii in (i, ctrl - 1 - i)
            ]
            x = [jnp.where(flip_y, y[1], y[0]) for y in x]
            x = jnp.where(flip_x, x[1], x[0])
            other = jnp.take_along_axis(x, index, axis=0, mode="promise_in_bounds")
            (stiff_out, mass_out)[f][i, j, :, lanes] = jnp.where(flip_z, other, x)[0:ctrl]
    exchange.drain()


RATE = (0.022, 0.04, 0.04)
LATENCY = (2.1, 3.4, 6.0)
TIMES = {"weigh": 0.62, "collect": 0.38, "expand": 0.27, "both": 0.48, "start": 0.03, "finish": 0.03, "final": 0.05}
WINDOW = 0.8
TAIL = 3.0
GRACE = -0.5


def exchange_plan(chunks, ctrl):
    free = [0.0, 0.0, 0.0]
    plan, ready, pending, begun, arrival = [], [], [], set(), {}
    folded = [set() for _ in range(chunks)]
    work = []
    for chunk in range(chunks):
        if 0 < chunk < chunks - 1:
            work += [("weigh", chunk), ("both", chunk)]
            continue
        work += [("weigh", chunk), ("collect", chunk)]
        work += [("expand", chunk + 1)] if chunk + 1 < chunks else []
    work.reverse()
    now = 0.0

    def step(name, chunk, m=None):
        nonlocal now
        plan.append((name, chunk, m))
        now += TIMES[name]

    def release(chunk, done):
        for m, move in enumerate(MOVES[chunk]):
            after = set(move.after)
            if (after & done if after else not done) and folded[chunk] >= after:
                followers = sum(m in other.after for other in MOVES[chunk])
                ready.append((1 if 0 not in move.axes else 0 if move.y == ENDS else 2, -followers, len(move.after) == 0, chunk, m))
        ready.sort()

    def held(chunk, m):
        followed = any(m in other.after for other in MOVES[chunk])
        return not followed and 1 in MOVES[chunk][m].axes and any(
            (c, n) not in begun
            for c in range(chunk)
            for n, move in enumerate(MOVES[c])
            if move.axes == (1,) and any(n in other.after for other in MOVES[c])
        )

    def foldable(chunk, m):
        after = set(MOVES[chunk][m].after)
        return all(
            (chunk, n) in begun
            for n, move in enumerate(MOVES[chunk])
            if n == m or 0 not in move.axes and (set(move.after) <= after or not move.after)
        )

    def issue():
        nonlocal now
        for item in list(ready):
            chunk, m = item[-2:]
            move = MOVES[chunk][m]
            if 0 in move.axes or not held(chunk, m) and max(free[a] for a in move.axes) <= now + (WINDOW if work else TAIL):
                ready.remove(item)
                begun.add((chunk, m))
                step("start", chunk, m)
                cost = move.points(ctrl) * 2 ** (len(move.axes) - 1)
                for a in move.axes:
                    free[a] = max(free[a], now) + cost * RATE[a]
                late = max(free[a] + LATENCY[a] for a in move.axes)
                arrival[chunk, m] = late
                members = group(chunk, m)
                if all((chunk, n) in begun for n in members):
                    late = max(arrival[chunk, n] for n in members)
                    heapq.heappush(pending, (late, chunk, members[-1]))

    while work or ready or pending:
        issue()
        able = sorted(
            p for p in pending if all(foldable(p[1], n) for n in group(p[1], p[2]))
        )
        near = [p for p in able if 2 not in MOVES[p[1]][p[2]].axes and p[0] <= now + GRACE]
        if work and not near:
            name, chunk = work.pop()
            step(name, chunk)
            if name in ("collect", "both"):
                release(chunk, set())
            continue
        if not able:
            now += WINDOW / 8
            continue
        late, chunk, m = near[0] if near else able[0]
        pending.remove((late, chunk, m))
        heapq.heapify(pending)
        now = max(now, late)
        step("finish", chunk, m)
        folded[chunk].update(group(chunk, m))
        release(chunk, set(group(chunk, m)))
        if len(folded[chunk]) == len(MOVES[chunk]):
            step("final", chunk)
    return plan


def apply_patch(u, diag, off, weight, orient, values, slopes):
    quad, ctrl = values.shape
    chunks = u.shape[3] // LANES
    points = quad * quad
    size = ctrl * ROWS
    forward, backward = plane_tables(values, slopes)
    scales = np.repeat(point_scales(values, slopes)[2][:, :, None], points, axis=2)
    vmem = pl.BlockSpec(memory_space=pltpu.VMEM)
    hbm = pl.BlockSpec(memory_space=pl.ANY)
    f32 = jnp.float32
    exchanged = [
        pltpu.VMEM((chunks, 2, 2, size, LANES), f32),
        pltpu.VMEM((chunks, 2, 2, ctrl, ctrl, LANES), f32),
    ]
    for planes in (INNER, ENDS, ALL):
        rows = len(span(planes, ctrl))
        exchanged.append(pltpu.VMEM((chunks, 2, 2, ctrl, rows, LANES), f32))
    for planes in (INNER, ENDS):
        rows = len(span(planes, ctrl))
        exchanged.append(pltpu.VMEM((chunks, 2, 2, 2, rows, LANES), f32))
    return pl.pallas_call(
        functools.partial(patch_kernel, values, slopes),
        out_shape=[pltpu.VMEM(u.shape, f32)] * 2,
        in_specs=[hbm] * 8,
        out_specs=[vmem, vmem],
        scratch_shapes=[
            pltpu.SMEM((3,), jnp.int32),
            pltpu.VMEM((chunks, ctrl, ctrl, ROWS, LANES), f32),
            pltpu.VMEM((14, quad, points), f32),
            pltpu.VMEM(forward.shape, jnp.bfloat16),
            pltpu.VMEM(backward.shape, f32),
            pltpu.VMEM((LANES, LANES), f32),
            pltpu.VMEM((2 * LANES, 2 * LANES), jnp.bfloat16),
            pltpu.VMEM((7 * quad, points, LANES), f32),
            pltpu.VMEM((ctrl, 3 * points, LANES), f32),
            pltpu.VMEM((ctrl, 4 * points, LANES), f32),
            pltpu.VMEM((2 * size, 12 * points), jnp.bfloat16),
            pltpu.VMEM((chunks, 2, ctrl, size, LANES), f32),
            exchanged,
            exchanged,
            pltpu.VMEM((sent_rows(ctrl), LANES), f32),
            pltpu.SemaphoreType.DMA((2,)),
            pltpu.SemaphoreType.DMA((4,)),
            pltpu.SemaphoreType.DMA,
            pltpu.SemaphoreType.DMA((sum(len(groups(c)) for c in range(chunks)),)),
        ],
        compiler_params=pltpu.CompilerParams(collective_id=0, has_side_effects=True),
        name="apply_patch",
    )(
        orient, u, diag, off, weight,
        jnp.asarray(scales), jnp.asarray(forward), jnp.asarray(backward),
    )


def store_kernel(stiff, mass, stiff_out, mass_out, sem):
    copies = [
        pltpu.make_async_copy(stiff, stiff_out, sem.at[0]),
        pltpu.make_async_copy(mass, mass_out, sem.at[1]),
    ]
    for copy in copies:
        copy.start()
    for copy in copies:
        copy.wait()


def store_results(stiff, mass):
    vmem = pl.BlockSpec(memory_space=pltpu.VMEM)
    hbm = pl.BlockSpec(memory_space=pl.ANY)
    return pl.pallas_call(
        store_kernel,
        out_shape=[jax.ShapeDtypeStruct(stiff.shape, stiff.dtype)] * 2,
        in_specs=[vmem, vmem],
        out_specs=[hbm, hbm],
        scratch_shapes=[pltpu.SemaphoreType.DMA((2,))],
        name="store_results",
    )(*(pltpu.with_memory_space_constraint(x, pltpu.VMEM) for x in (stiff, mass)))


def per_device(control_values, metric_diag, metric_off, mass_weight, orient):
    values, slopes = spline_tables(mass_weight.shape[0] // 2)
    stiff, mass = apply_patch(
        control_values, metric_diag, metric_off, mass_weight, orient.reshape(3), values, slopes
    )
    return tuple(store_results(stiff, mass))


def solution(mesh):
    in_specs = (
        P("px", "py", "pz", None),
        P(None, "px", ("py", "pz")),
        P(None, "px", ("py", "pz")),
        P("px", ("py", "pz")),
        P("px", "py", "pz", None),
    )
    out_specs = (P("px", "py", "pz", None), P("px", "py", "pz", None))
    return jax.shard_map(
        per_device, mesh=mesh, in_specs=in_specs, out_specs=out_specs, check_vma=False
    )
```
